256 devices in a mesh: dp: 16 (over x_lo, y, core), ctx: 16 (over x_hi, z).
Axes of the slice: x: 4 (x_hi: 2, x_lo: 2; x = x_hi * 2 + x_lo), y: 4, z: 8, core: 2. Of those that a mesh axis runs over, the one named last changes fastest.
Arguments:
- query: bfloat16 [16, 2048, 2048], P('dp', 'ctx'), may hold values from -16 to 16
- keys: bfloat16 [16, 2048, 2048], P('dp', 'ctx'), may hold values from -16 to 16
- values: bfloat16 [16, 2048, 2048], P('dp', 'ctx'), may hold values from -6 to 6
- codes: int32 [16, 2048, 4], P('dp', 'ctx'), may hold values from 0 to 2047
- w_in: bfloat16 [2048, 1024], replicated, may hold values from -0.125 to 0.125
- table: bfloat16 [2048, 1024], replicated, may hold values from -0.67 to 0.67
- gain: float32 [1024], replicated, may hold values from 0.5 to 1.5
- w_qkv: bfloat16 [1024, 1536], P('dp'), may hold values from -0.140625 to 0.140625
- w_out: bfloat16 [512, 1024], P('dp'), may hold values from -0.25 to 0.25
Outputs:
- grad_qkv: float32 [1024, 1536], P('dp')
- grad_out: float32 [512, 1024], P('dp')
The draws below stay inside these ranges and needn't reach their ends.
All inputs are finite; a program needn't handle non-finite values.
Results may differ from the reference program's by a relative error of at most 0.01.
Values may be sent and summed in bfloat16 or wider, within the bound.
No kernel may reach another device: no remote copies, remote signals or barrier semaphores. Data moves between devices by JAX's collectives and lax.ppermute only.
A program may use at most 128 MiB of HBM per device.

```python
import math
import jax
import jax.numpy as jnp
from jax import lax

HEADS = 16
HEAD_DIM = 128
DEPTH_DIM = 1024
DEPTH_HEADS = 8
DEPTH_HEAD = 64
CODES = 2048
CB = 4
TOK_DEV = 128
HD = 2048
DH = 512
DIALOGS = 16
SEQ = 2048
N_CTX = 16


def paired_draw(key):
    query_key = jax.random.fold_in(key, 71)
    keys_key = jax.random.fold_in(key, 72)
    query = jnp.clip(jax.random.normal(query_key, (DIALOGS, SEQ, HD), jnp.float32), -4.0, 4.0)
    keyset = jnp.clip(jax.random.normal(keys_key, (DIALOGS, SEQ, HD), jnp.float32), -4.0, 4.0)
    return (query.astype(jnp.bfloat16), keyset.astype(jnp.bfloat16))


def draw_query(key, part):
    return paired_draw(key)[0]


def draw_keys(key, part):
    return paired_draw(key)[1]


def draw_table(key, part):
    result = jnp.clip(0.094 * jax.random.normal(jax.random.fold_in(key, 94), (CODES, DEPTH_DIM), jnp.float32), -0.6, 0.6)
    return result.astype(jnp.bfloat16)


def draw_w_qkv(key, part):
    head_width = DEPTH_HEADS * DEPTH_HEAD
    base = jnp.clip(jax.random.normal(jax.random.fold_in(key, 95), (DEPTH_DIM, 3 * head_width), jnp.float32), -4.5, 4.5)
    result = base / DEPTH_DIM ** 0.5
    return result.astype(jnp.bfloat16)


def place_ends(drawn, key, least, top_value):
    longest = drawn.shape.index(max(drawn.shape))
    spots = []
    for shift in (0, 1):
        where = [jax.random.randint(jax.random.fold_in(key, axis), (), 0, length) for axis, length in enumerate(drawn.shape)]
        where[longest] = (where[longest] + shift) % drawn.shape[longest]
        spots.append(tuple(where))
    return drawn.at[spots[0]].set(least).at[spots[1]].set(top_value)


def shard_levels(own_key, shape, pieces, smallest, high):
    loudness, own = 1.0, jax.random.fold_in(own_key, 6)
    for axis_at, shards_of in pieces:
        draws = jnp.exp(jax.random.uniform(jax.random.fold_in(own, axis_at), (shards_of,), jnp.float32, smallest / len(pieces), high / len(pieces)))
        loudness = loudness * jnp.repeat(draws, shape[axis_at] // shards_of).reshape([-1 if axis == axis_at else 1 for axis in range(len(shape))])
    return loudness


def noise(stream_key, shape, scale, most, split=(), kind=jnp.bfloat16):
    drawn = scale * jax.random.normal(stream_key, shape, jnp.float32)
    if split:
        drawn = drawn * shard_levels(stream_key, shape, split, -0.22, 0.18)
    return jnp.clip(drawn, -most, most).astype(kind)


def setup_inputs(seed: int = 0) -> dict:
    seeds = jax.random.split(jax.random.key(seed), 10)
    return {
        "query": draw_query(jax.random.fold_in(seeds[9], 71), 0),
        "keys": draw_keys(jax.random.fold_in(seeds[9], 71), 0),
        "values": noise(seeds[2], (DIALOGS, SEQ, HD), 1.0, 6.0, ((0, 16), (1, 16))),
        "codes": place_ends(jax.random.randint(seeds[3], (DIALOGS, SEQ, CB), 0, CODES), jax.random.fold_in(seeds[3], 1), 0, CODES - 1).astype(jnp.int32),
        "w_in": noise(seeds[4], (HD, DEPTH_DIM), HD ** -0.5, 0.125),
        "table": draw_table(jax.random.fold_in(seeds[9], 71), 0),
        "gain": jnp.clip(1.0 + 0.1 * jax.random.normal(seeds[6], (DEPTH_DIM,), jnp.float32), 0.5, 1.5),
        "w_qkv": draw_w_qkv(jax.random.fold_in(seeds[9], 71), 0),
        "w_out": noise(seeds[8], (DH, DEPTH_DIM), DH ** -0.5, 0.25, ((0, 16),)),
    }


epsilon = 1e-06
masked_score = -1e+30

def normalize(values_in):
    return values_in * lax.rsqrt(lax.optimization_barrier(jnp.mean(values_in * values_in, axis=-1, keepdims=True)) + epsilon)

def causal_head_block(query_heads, key_heads, value_heads, first_row, block_rows):
    key_total = key_heads.shape[0]
    scores = jnp.einsum('qhd,khd->hqk', query_heads.astype(jnp.float32), key_heads.astype(jnp.float32)) / math.sqrt(HEAD_DIM)
    row_ids = first_row + jnp.arange(block_rows, dtype=jnp.int32)
    col_ids = jnp.arange(key_total, dtype=jnp.int32)
    allowed = col_ids[None, :] <= row_ids[:, None]
    scores = jnp.where(allowed[None], scores, masked_score)
    highest = lax.optimization_barrier(jnp.max(scores, axis=-1, keepdims=True))
    weights = jnp.where(allowed[None], jnp.exp(scores - highest), 0.0)
    totals = lax.optimization_barrier(jnp.sum(weights, axis=-1))
    rounded = lax.optimization_barrier(weights.astype(jnp.bfloat16)).astype(jnp.float32)
    mixed = jnp.einsum('hqk,khd->hqd', rounded, value_heads.astype(jnp.float32)) / totals[..., None]
    return jnp.transpose(mixed, (1, 0, 2)).reshape(block_rows, -1).astype(jnp.bfloat16)

def temporal_dialogue(query_rows, key_rows, value_rows):
    query_heads = query_rows.reshape(SEQ, HEADS, HEAD_DIM)
    key_heads = key_rows.reshape(SEQ, HEADS, HEAD_DIM)
    value_heads = value_rows.reshape(SEQ, HEADS, HEAD_DIM)
    block_rows = min(512, SEQ)
    block_count = SEQ // block_rows

    def one_block(index):
        first_row = (index * block_rows).astype(jnp.int32)
        query_block = lax.dynamic_slice_in_dim(query_heads, first_row, block_rows, 0)
        return causal_head_block(query_block, key_heads, value_heads, first_row, block_rows)
    return lax.map(one_block, jnp.arange(block_count, dtype=jnp.int32)).reshape(SEQ, HD)

def depth_terms(attended, frame_codes, w_in, table, gain, w_qkv, w_out, weight):
    frame_count = attended.shape[0]
    positions = frame_codes.shape[1]
    width = table.shape[1]
    head_width = w_out.shape[0]
    total_rows = frame_count * positions
    hidden = jnp.dot(attended, w_in, preferred_element_type=jnp.float32)
    embedded = jnp.take(table, frame_codes[:, :positions - 1], axis=0).astype(jnp.float32)
    depth_in = jnp.concatenate([hidden[:, None, :], hidden[:, None, :] + embedded], axis=1)
    normed = (normalize(depth_in) * gain).astype(jnp.bfloat16).reshape(total_rows, width)
    qkv_rounded = jnp.dot(normed, w_qkv, preferred_element_type=jnp.float32).astype(jnp.bfloat16)
    qkv_wide = lax.optimization_barrier(qkv_rounded).astype(jnp.float32)
    qkv_wide = qkv_wide.reshape(frame_count, positions, 3, DEPTH_HEADS, DEPTH_HEAD)
    query_part = qkv_wide[:, :, 0]
    key_part = qkv_wide[:, :, 1]
    value_part = qkv_wide[:, :, 2]
    scale = 1.0 / math.sqrt(DEPTH_HEAD)
    causal = jnp.arange(positions)[None, :] <= jnp.arange(positions)[:, None]
    scores = jnp.einsum('rqhd,rkhd->rhqk', query_part, key_part) * scale
    scores = jnp.where(causal[None, None], scores, masked_score)
    probs = jax.nn.softmax(scores, axis=-1)
    mixed = jnp.einsum('rhqk,rkhd->rqhd', probs, value_part).reshape(total_rows, head_width)
    mixed_rounded = mixed.astype(jnp.bfloat16)
    resid = depth_in.reshape(total_rows, width) + jnp.dot(mixed_rounded, w_out, preferred_element_type=jnp.float32)
    inverse = lax.rsqrt(lax.optimization_barrier(jnp.mean(resid * resid, axis=-1, keepdims=True)) + epsilon)
    normal_out = resid * inverse
    logits = jnp.dot(normal_out.astype(jnp.bfloat16), table.T, preferred_element_type=jnp.float32)
    targets = frame_codes.reshape(total_rows)
    highest = lax.optimization_barrier(jnp.max(logits, axis=-1, keepdims=True))
    exped = jnp.exp(logits - highest)
    totals = lax.optimization_barrier(jnp.sum(exped, axis=-1, keepdims=True))
    onehot = jnp.arange(logits.shape[1], dtype=jnp.int32)[None, :] == targets[:, None]
    grad_logits = ((exped / totals - onehot.astype(jnp.float32)) * weight).astype(jnp.bfloat16)
    grad_normal = jnp.dot(grad_logits, table, preferred_element_type=jnp.float32)
    grad_resid = inverse * (grad_normal - normal_out * lax.optimization_barrier(jnp.mean(grad_normal * normal_out, axis=-1, keepdims=True)))
    resid_rounded = grad_resid.astype(jnp.bfloat16)
    out_grad = jnp.dot(mixed_rounded.T, resid_rounded, preferred_element_type=jnp.float32)
    grad_mixed = jnp.dot(resid_rounded, w_out.T, preferred_element_type=jnp.float32)
    grad_mixed = grad_mixed.reshape(frame_count, positions, DEPTH_HEADS, DEPTH_HEAD)
    grad_value = jnp.einsum('rhqk,rqhd->rkhd', probs, grad_mixed)
    grad_probs = jnp.einsum('rqhd,rkhd->rhqk', grad_mixed, value_part)
    grad_scores = probs * (grad_probs - lax.optimization_barrier(jnp.sum(grad_probs * probs, axis=-1, keepdims=True))) * scale
    grad_query = jnp.einsum('rhqk,rkhd->rqhd', grad_scores, key_part)
    grad_key = jnp.einsum('rhqk,rqhd->rkhd', grad_scores, query_part)
    grad_joined = jnp.stack([grad_query, grad_key, grad_value], axis=2).reshape(total_rows, 3 * head_width)
    qkv_grad = jnp.dot(normed.T, grad_joined.astype(jnp.bfloat16), preferred_element_type=jnp.float32)
    return (qkv_grad, out_grad)

def reference(query, keys, values, codes, w_in, table, gain, w_qkv, w_out):
    attended = lax.map(lambda triple: temporal_dialogue(triple[0], triple[1], triple[2]), (query, keys, values))
    shards = attended.reshape(DIALOGS * N_CTX, TOK_DEV, HD)
    code_shards = codes.reshape(DIALOGS * N_CTX, TOK_DEV, CB)
    weight = 1.0 / DIALOGS

    def absorb(carry, item):
        qkv_grad, out_grad = depth_terms(item[0], item[1], w_in, table, gain, w_qkv, w_out, weight)
        return ((carry[0] + qkv_grad, carry[1] + out_grad), None)
    start_state = (jnp.zeros(w_qkv.shape, jnp.float32), jnp.zeros(w_out.shape, jnp.float32))
    (grad_qkv, grad_out), _ = lax.scan(absorb, start_state, (shards, code_shards))
    return (grad_qkv, grad_out)
```

```python
import functools
import math

import jax
import jax.numpy as jnp
from jax import lax
from jax.experimental import pallas as pl
from jax.experimental.pallas import tpu as pltpu
from jax.sharding import Mesh
from jax.sharding import PartitionSpec as P

HEAD_DIM = 128
DEPTH_HEAD = 64
DP = ("dp_0", "dp_1", "dp_2")
CTX = ("ctx_0", "ctx_1")
PLANE = ("dp_0", "dp_1", "ctx_0")

bf16, f32 = jnp.bfloat16, jnp.float32
NEG = -1e30
EPS = 1e-6
NT = (((1,), (1,)), ((), ()))


def dot(a, b):
    return jnp.dot(a, b, preferred_element_type=f32)


def dot_nt(a, b):
    return lax.dot_general(a, b, NT, preferred_element_type=f32)


def attend_body(x_ref, o_ref, *, step):
    blocks, _, rows, dim = x_ref.shape
    for i in range(0, blocks, step):
        seen = i + step
        q = x_ref[i:seen, 0].reshape(step * rows, dim)
        k = x_ref[0:seen, 1].reshape(seen * rows, dim)
        v = x_ref[0:seen, 2].reshape(seen * rows, dim)
        s = dot_nt(q, k) * (1.0 / math.sqrt(dim))
        shape = (step * rows, step * rows)
        ok = lax.broadcasted_iota(jnp.int32, shape, 1) <= lax.broadcasted_iota(jnp.int32, shape, 0)
        last = jnp.where(ok, s[:, i * rows :], NEG)
        s = last if i == 0 else jnp.concatenate([s[:, : i * rows], last], axis=1)
        p = jnp.exp(s - jnp.max(s, axis=1, keepdims=True))
        total = jnp.sum(p, axis=1, keepdims=True)
        out = dot(p.astype(bf16), v) / total
        o_ref[i:seen] = out.astype(bf16).reshape(step, rows, dim)


def embed_body(codes_ref, table_ref, o_ref, hot_ref):
    count, frames, width = o_ref.shape
    entries = table_ref.shape[0]
    ids = lax.broadcasted_iota(jnp.int32, (frames, entries), 1)
    for c in range(count):
        hot_ref[c * frames : (c + 1) * frames] = (
            (ids == codes_ref[:, c : c + 1]).astype(f32).astype(bf16)
        )
    tile = 256

    @pl.loop(0, width // tile)
    def _(j):
        cols = pl.ds(pl.multiple_of(j * tile, tile), tile)
        rows = dot(hot_ref[...], table_ref[:, cols])
        o_ref[:, :, cols] = rows.astype(bf16).reshape(count, frames, tile)


def put_split(ref, k, frames, count, term):
    high = term.astype(bf16)
    ref[k * frames : (k + 1) * frames] = high
    ref[(count + k) * frames : (count + k + 1) * frames] = (term - high.astype(f32)).astype(bf16)


def head_sums(ref, rows, heads_block, store):
    width = heads_block.shape[0]
    for j in range(ref.shape[1] // width):
        cols = slice(j * width, (j + 1) * width)
        store(cols, dot(ref[:rows, cols], heads_block) + dot(ref[rows:, cols], heads_block))


def same_head(width, head):
    r = lax.broadcasted_iota(jnp.int32, (width, width), 0) // head
    c = lax.broadcasted_iota(jnp.int32, (width, width), 1) // head
    return (r == c).astype(f32).astype(bf16)


def pairs_of(positions):
    return [(c, e) for c in range(positions) for e in range(c + 1)]


def depth_body(
    place_ref, att_ref, emb_ref, codes_ref, gain_ref, w_in_hbm, table_hbm, w0_hbm, w1_hbm, w2_hbm, w3_hbm,
    t0_hbm, t1_hbm, t2_hbm, t3_hbm, keep_ref, send_ref,
    w_in_ref, table_ref, w_ref, w_out_ref, x_ref, n_ref, n_t_ref, qkv_ref, term_ref, s_ref, p_ref, mix_ref, mix_t_ref, inv_ref,
    logit_ref, g_ref, dr_ref, dqkv_ref, stage_ref, sems, in_sems, table_sem,
    *, weight, head,
):
    frames, positions = codes_ref.shape
    width = x_ref.shape[1]
    entries = table_ref.shape[0]
    dh = w_out_ref.shape[0]
    owners, _, rows_qkv, _ = stage_ref.shape
    rows_out = rows_qkv // 2
    half = width // 2
    tile = 256
    side = place_ref[2]
    z_ref = x_ref
    dz_ref = logit_ref.at[:, :width]
    dmix_ref = logit_ref.at[:, width : width + dh]
    row = lambda c: pl.ds(c * frames, frames)

    tile_cols = lambda j: pl.ds(pl.multiple_of(j * tile, tile), tile)
    load_in = lambda j: pltpu.make_async_copy(
        w_in_hbm.at[:, tile_cols(j)], w_in_ref.at[:, tile_cols(j)], in_sems.at[j]
    )
    load_table = pltpu.make_async_copy(table_hbm, table_ref, table_sem)
    for j in range(width // tile):
        load_in(j).start()
    loads = []
    mine, twins = (w0_hbm, w1_hbm, w2_hbm, w3_hbm), (t0_hbm, t1_hbm, t2_hbm, t3_hbm)
    for twin, refs in enumerate((mine, twins)):
        for back, ref in enumerate(refs):
            for plane in range(2):
                at = (place_ref[0] + plane) % 2
                at = at * len(refs) + (place_ref[1] + len(refs) - back) % len(refs)
                at = at * 2 + (side + twin) % 2
                rows = pl.ds(pl.multiple_of(at * rows_qkv, rows_qkv), rows_qkv)
                loads.append(pltpu.make_async_copy(ref.at[plane], w_ref.at[rows], sems.at[len(loads)]))
                loads[-1].start()
    load_table.start()
    att = jnp.concatenate([att_ref[h] for h in range(att_ref.shape[0])], axis=1)

    @pl.loop(0, width // tile)
    def _(j):
        cols = pl.ds(pl.multiple_of(j * tile, tile), tile)
        load_in(j).wait()
        hidden = dot(att, w_in_ref[:, cols])
        x_ref[row(0), cols] = hidden
        for c in range(1, positions):
            x_ref[row(c), cols] = hidden + emb_ref[c - 1, :, cols].astype(f32)

    for c in range(positions):
        x = x_ref[row(c), :]
        scale = lax.rsqrt(jnp.mean(x * x, axis=1, keepdims=True) + EPS)
        normed = (x * scale * gain_ref[...]).astype(bf16)
        n_ref[row(c), :] = normed
        n_t_ref[:, row(c)] = normed.T

    for load in loads:
        load.wait()
    for d in range(2 * owners):
        for k in range(2):
            w_out_ref[d * rows_out : (d + 1) * rows_out, k * half : (k + 1) * half] = w_ref[
                d * rows_qkv + k * rows_out : d * rows_qkv + (k + 1) * rows_out, 3 * dh :
            ]

    @pl.loop(0, 3 * dh // tile)
    def _(j):
        cols = pl.ds(pl.multiple_of(j * tile, tile), tile)
        qkv_ref[:, cols] = dot(n_ref[...], w_ref[:, cols]).astype(bf16)

    block = same_head(tile, head)
    scale = 1.0 / math.sqrt(head)
    pairs = pairs_of(positions)
    part = lambda c, k: qkv_ref[row(c), k * dh : (k + 1) * dh].astype(f32)
    count = len(pairs)
    pair = lambda c, e: pl.ds(pairs.index((c, e)) * frames, frames)

    def store_scores(cols, values):
        s_ref[:, cols] = values * scale

    for k, (c, e) in enumerate(pairs):
        put_split(term_ref, k, frames, count, part(c, 0) * part(e, 1))
    head_sums(term_ref, count * frames, block, store_scores)
    for c in range(positions):
        scores = [s_ref[pair(c, e), :] for e in range(c + 1)]
        top = functools.reduce(jnp.maximum, scores)
        raised = [jnp.exp(s - top) for s in scores]
        fraction = 1.0 / functools.reduce(jnp.add, raised)
        mixed = jnp.zeros((frames, dh), f32)
        for e in range(c + 1):
            p = raised[e] * fraction
            p_ref[pair(c, e), :] = p
            mixed = mixed + p * part(e, 2)
        mixed = mixed.astype(bf16)
        mix_ref[row(c), :] = mixed
        mix_t_ref[:, row(c)] = mixed.T

    @pl.loop(0, width // tile)
    def _(j):
        cols = pl.ds(pl.multiple_of(j * tile, tile), tile)
        z_ref[:, cols] = x_ref[:, cols] + dot(mix_ref[...], w_out_ref[:, cols])

    for c in range(positions):
        r = z_ref[row(c), :]
        inv = lax.rsqrt(jnp.mean(r * r, axis=1, keepdims=True) + EPS)
        inv_ref[row(c), :] = jnp.broadcast_to(inv, (frames, inv_ref.shape[1]))
        z = r * inv
        z_ref[row(c), :] = z
        dr_ref[row(c), :] = z.astype(bf16)

    load_table.wait()

    @pl.loop(0, entries // tile)
    def _(j):
        cols = pl.ds(pl.multiple_of(j * tile, tile), tile)
        logit_ref[:, cols] = dot_nt(dr_ref[...], table_ref[cols, :])

    ids = lax.broadcasted_iota(jnp.int32, (frames, entries), 1)
    for c in range(positions):
        s = logit_ref[row(c), :]
        e = jnp.exp(s - jnp.max(s, axis=1, keepdims=True))
        total = jnp.sum(e, axis=1, keepdims=True)
        hit = jnp.where(ids == codes_ref[:, c : c + 1], weight, 0.0)
        g_ref[row(c), :] = (e * (weight / total) - hit).astype(bf16)

    @pl.loop(0, width // tile)
    def _(j):
        cols = pl.ds(pl.multiple_of(j * tile, tile), tile)
        dz_ref[:, cols] = dot(g_ref[...], table_ref[:, cols])

    for c in range(positions):
        dz, z = dz_ref[row(c), :], z_ref[row(c), :]
        along = jnp.mean(dz * z, axis=1, keepdims=True)
        dr_ref[row(c), :] = (inv_ref[row(c), 0:1] * (dz - z * along)).astype(bf16)

    for j in range(width // tile):
        part_out = dot(mix_t_ref[...], dr_ref[:, j * tile : (j + 1) * tile]).astype(bf16)
        stage_ref[:, :, 0:rows_out, :] = part_out.reshape(owners, 2, rows_out, tile)
        k, at = divmod(j * tile, half)
        rows = slice(k * rows_out, (k + 1) * rows_out)
        cols = slice(3 * dh + at, 3 * dh + at + tile)
        keep_ref[:, rows, cols] = stage_ref[:, side, 0:rows_out, :]
        send_ref[:, rows, cols] = stage_ref[:, 1 - side, 0:rows_out, :]

    @pl.loop(0, dh // tile)
    def _(j):
        cols = pl.ds(pl.multiple_of(j * tile, tile), tile)
        dmix_ref[:, cols] = dot_nt(dr_ref[...], w_out_ref[cols, :])

    def store_plain(cols, values):
        s_ref[:, cols] = values

    for k, (c, e) in enumerate(pairs):
        put_split(term_ref, k, frames, count, dmix_ref[row(c), :] * part(e, 2))
    head_sums(term_ref, count * frames, block, store_plain)
    dk = [jnp.zeros((frames, dh), f32) for _ in range(positions)]
    dv = [jnp.zeros((frames, dh), f32) for _ in range(positions)]
    for c in range(positions):
        dm = dmix_ref[row(c), :]
        probs = [p_ref[pair(c, e), :] for e in range(c + 1)]
        dprobs = [s_ref[pair(c, e), :] for e in range(c + 1)]
        along = functools.reduce(jnp.add, [d * p for d, p in zip(dprobs, probs)])
        q = part(c, 0)
        dq = jnp.zeros((frames, dh), f32)
        for e in range(c + 1):
            ds = probs[e] * (dprobs[e] - along) * scale
            dq = dq + ds * part(e, 1)
            dk[e] = dk[e] + ds * q
            dv[e] = dv[e] + probs[e] * dm
        dqkv_ref[row(c), 0:dh] = dq.astype(bf16)
    for c in range(positions):
        dqkv_ref[row(c), dh : 2 * dh] = dk[c].astype(bf16)
        dqkv_ref[row(c), 2 * dh :] = dv[c].astype(bf16)

    @pl.loop(0, 3 * dh // tile)
    def _(j):
        cols = pl.ds(pl.multiple_of(j * tile, tile), tile)
        part_qkv = dot(n_t_ref[...], dqkv_ref[:, cols]).astype(bf16)
        stage_ref[...] = part_qkv.reshape(owners, 2, rows_qkv, tile)
        keep_ref[:, :, cols] = stage_ref[:, side]
        send_ref[:, :, cols] = stage_ref[:, 1 - side]


def pack_body(query_ref, keys_ref, values_ref, o_ref):
    for d in range(o_ref.shape[0]):
        cols = slice(d * o_ref.shape[3], (d + 1) * o_ref.shape[3])
        for k, ref in enumerate((query_ref, keys_ref, values_ref)):
            o_ref[d, k] = ref[0, :, cols]


def add_cut_body(a_ref, b_ref, o_ref):
    width = o_ref.shape[3]
    for k in range(o_ref.shape[1]):
        cols = slice(k * width, (k + 1) * width)
        o_ref[:, k] = (a_ref[:, :, cols].astype(f32) + b_ref[:, :, cols].astype(f32)).astype(bf16)


def fold_cut_body(x_ref, o_ref):
    width = o_ref.shape[2]
    for j in range(o_ref.shape[0]):
        cols = slice(j * width, (j + 1) * width)
        o_ref[j] = functools.reduce(
            jnp.add, [x_ref[d, :, cols].astype(f32) for d in range(x_ref.shape[0])]
        ).astype(bf16)


def fold_copy_body(x_ref, o_ref):
    total = functools.reduce(jnp.add, [x_ref[d].astype(f32) for d in range(x_ref.shape[0])])
    for j in range(o_ref.shape[0]):
        o_ref[j] = total.astype(bf16)


def lay_out_body(x_ref, qkv_ref, out_ref):
    width = x_ref.shape[2]
    rows_out, cols_out = out_ref.shape
    for j in range(x_ref.shape[0]):
        part, at = x_ref[j].astype(f32), j * width
        if at < qkv_ref.shape[1]:
            qkv_ref[:, at : at + width] = part
        else:
            at -= qkv_ref.shape[1]
            for k in range(2):
                cols = slice(k * (cols_out // 2) + at, k * (cols_out // 2) + at + width)
                out_ref[:, cols] = part[k * rows_out : (k + 1) * rows_out]


VMEM = pl.BlockSpec(memory_space=pltpu.VMEM)
SMEM = pl.BlockSpec(memory_space=pltpu.SMEM)
ANY = pl.BlockSpec(memory_space=pl.ANY)


def kernel(body, outs, name, flops, in_specs=None, scratch=(), room=None):
    many = isinstance(outs, (list, tuple))
    every = list(outs) if many else [outs]
    size = sum(math.prod(o.shape) * o.dtype.itemsize for o in every)

    def call(*args):
        return pl.pallas_call(
            body,
            out_shape=every if many else outs,
            in_specs=in_specs or [VMEM] * len(args),
            out_specs=[VMEM] * len(every) if many else VMEM,
            scratch_shapes=list(scratch),
            cost_estimate=pl.CostEstimate(
                flops=flops,
                bytes_accessed=size + sum(math.prod(a.shape) * a.dtype.itemsize for a in args),
                transcendentals=0,
            ),
            compiler_params=pltpu.CompilerParams(vmem_limit_bytes=room),
            name=name,
        )(*args)

    return call


def shape(dims, dtype=bf16):
    return jax.ShapeDtypeStruct(tuple(dims), dtype)


def to_all(x, axis):
    return lax.all_to_all(x, axis, 0, 0, tiled=True)


def turned(x, axis, k):
    n = lax.axis_size(axis)
    return lax.ppermute(x, axis, [(i, (i + k) % n) for i in range(n)])


def depth_call(weight, place, attended, embedded, codes, gain, w_in, table, weights):
    frames, positions = codes.shape
    width, entries, rows = w_in.shape[1], table.shape[0], frames * positions
    dh = (weights[0].shape[2] - width // 2) // 3
    _, share, columns = weights[0].shape
    owners = len(weights)
    cut = shape((owners, share, columns))
    pairs = len(pairs_of(positions)) * frames
    return kernel(
        functools.partial(depth_body, weight=weight, head=DEPTH_HEAD),
        (cut, cut),
        "depth",
        11 * 10**9,
        room=40 << 20,
        in_specs=[SMEM] + [VMEM] * 4 + [ANY] * 10,
        scratch=[
            pltpu.VMEM(w_in.shape, bf16),
            pltpu.VMEM(table.shape, bf16),
            pltpu.VMEM((width, columns), bf16),
            pltpu.VMEM((dh, width), bf16),
            pltpu.VMEM((rows, width), f32),
            pltpu.VMEM((rows, width), bf16),
            pltpu.VMEM((width, rows), bf16),
            pltpu.VMEM((rows, 3 * dh), bf16),
            pltpu.VMEM((2 * pairs, dh), bf16),
            pltpu.VMEM((pairs, dh), f32),
            pltpu.VMEM((pairs, dh), f32),
            pltpu.VMEM((rows, dh), bf16),
            pltpu.VMEM((dh, rows), bf16),
            pltpu.VMEM((rows, 128), f32),
            pltpu.VMEM((rows, entries), f32),
            pltpu.VMEM((rows, entries), bf16),
            pltpu.VMEM((rows, width), bf16),
            pltpu.VMEM((rows, 3 * dh), bf16),
            pltpu.VMEM((owners, 2, share, 256), bf16),
            pltpu.SemaphoreType.DMA((2 * owners,)),
            pltpu.SemaphoreType.DMA((width // 256,)),
            pltpu.SemaphoreType.DMA,
        ],
    )(place, attended, embedded, codes, gain.reshape(1, width), w_in, table, *weights)


def local(query, keys, values, codes, w_in, table, gain, w_qkv, w_out):
    parts = lax.axis_size(CTX)
    frames, positions = codes.shape[1:]
    width, dh = w_in.shape[1], w_out.shape[0] * lax.axis_size(DP)
    entries = table.shape[0]
    place = jnp.stack([lax.axis_index(name) for name in DP])

    packed = kernel(pack_body, shape((parts, 3, frames, HEAD_DIM)), "pack", 1 << 20)(
        query, keys, values
    )
    w_qkv, w_out, packed = lax.optimization_barrier((w_qkv, w_out, packed))
    both = jnp.concatenate(
        [w_qkv, jnp.concatenate([w_out[:, : width // 2], w_out[:, width // 2 :]], axis=0)], axis=1
    )
    pair = jnp.stack([both, turned(both, "dp_0", 1)])
    near = [pair] + [turned(pair, "dp_1", k) for k in range(1, lax.axis_size("dp_1"))]

    moved = to_all(packed, CTX)
    embedded = kernel(
        embed_body,
        shape((positions - 1, frames, width)),
        "embed",
        2 * (positions - 1) * frames * entries * width,
        room=10 << 20,
        scratch=[pltpu.VMEM(((positions - 1) * frames, entries), bf16)],
    )(codes[0], table)

    heads = kernel(
        functools.partial(attend_body, step=2),
        shape((parts, frames, HEAD_DIM)),
        "attend",
        4 * (parts * frames) ** 2 * HEAD_DIM,
        room=24 << 20,
    )(moved)
    attended = to_all(heads, CTX)
    near, heads = lax.optimization_barrier((near, heads))
    weights = near + [turned(w, "dp_2", 1) for w in near]

    keep, send = depth_call(
        1.0 / lax.axis_size(DP), place, attended, embedded, codes[0], gain, w_in, table, weights
    )
    swapped = turned(send, "dp_2", 1)
    owners, rows, columns = keep.shape
    planes, lane = lax.axis_size("ctx_0"), columns // parts
    halves = shape((owners, planes, rows, columns // planes))
    chip_sum = kernel(add_cut_body, halves, "chip_sum", 1 << 22, room=16 << 20)(keep, swapped)
    chip_sum = chip_sum.reshape(owners * planes, rows, columns // planes)
    plane_sum = kernel(
        fold_cut_body, shape((parts // planes, rows, lane)), "plane_sum", 1 << 22, room=8 << 20
    )(to_all(chip_sum, PLANE))
    whole_sum = kernel(fold_copy_body, shape((parts, rows, lane)), "whole_sum", 1 << 20, room=4 << 20)(
        to_all(plane_sum, "ctx_1")
    )
    return kernel(
        lay_out_body, (shape(w_qkv.shape, f32), shape(w_out.shape, f32)), "lay_out", 1 << 20, room=4 << 20
    )(to_all(whole_sum, CTX))


def solution(mesh):
    torus = Mesh(mesh.devices.reshape(2, 4, 2, 2, 8), DP + CTX)
    frames = P(DP, CTX, None)
    in_specs = (frames, frames, frames, frames, P(), P(), P(), P(DP, None), P(DP, None))
    out_specs = (P(DP, None), P(DP, None))
    return jax.shard_map(local, mesh=torus, in_specs=in_specs, out_specs=out_specs, check_vma=False)
```

```python
import functools
import math

import jax
import jax.numpy as jnp
from jax import lax
from jax.experimental import pallas as pl
from jax.experimental.pallas import tpu as pltpu
from jax.sharding import Mesh
from jax.sharding import PartitionSpec as P

HEAD_DIM = 128
DEPTH_HEAD = 64
DP = ("dp_0", "dp_1", "dp_2")
CTX = ("ctx_0", "ctx_1")
PLANE = ("dp_0", "dp_1", "ctx_0")

bf16, f32 = jnp.bfloat16, jnp.float32
NEG = -1e30
EPS = 1e-6
NT = (((1,), (1,)), ((), ()))


def dot(a, b):
    return jnp.dot(a, b, preferred_element_type=f32)


def dot_nt(a, b):
    return lax.dot_general(a, b, NT, preferred_element_type=f32)


def attend_body(x_ref, o_ref, *, step):
    blocks, _, rows, dim = x_ref.shape
    for i in range(0, blocks, step):
        seen = i + step
        q = x_ref[i:seen, 0].reshape(step * rows, dim)
        k = x_ref[0:seen, 1].reshape(seen * rows, dim)
        v = x_ref[0:seen, 2].reshape(seen * rows, dim)
        s = dot_nt(q, k) * (1.0 / math.sqrt(dim))
        shape = (step * rows, step * rows)
        ok = lax.broadcasted_iota(jnp.int32, shape, 1) <= lax.broadcasted_iota(jnp.int32, shape, 0)
        last = jnp.where(ok, s[:, i * rows :], NEG)
        s = last if i == 0 else jnp.concatenate([s[:, : i * rows], last], axis=1)
        p = jnp.exp(s - jnp.max(s, axis=1, keepdims=True))
        total = jnp.sum(p, axis=1, keepdims=True)
        out = dot(p.astype(bf16), v) / total
        o_ref[i:seen] = out.astype(bf16).reshape(step, rows, dim)


def embed_body(codes_ref, table_ref, o_ref, hot_ref):
    count, frames, width = o_ref.shape
    entries = table_ref.shape[0]
    ids = lax.broadcasted_iota(jnp.int32, (frames, entries), 1)
    for c in range(count):
        hot_ref[c * frames : (c + 1) * frames] = (
            (ids == codes_ref[:, c : c + 1]).astype(f32).astype(bf16)
        )
    tile = 256

    @pl.loop(0, width // tile)
    def _(j):
        cols = pl.ds(pl.multiple_of(j * tile, tile), tile)
        rows = dot(hot_ref[...], table_ref[:, cols])
        o_ref[:, :, cols] = rows.astype(bf16).reshape(count, frames, tile)


def put_split(ref, k, frames, count, term):
    high = term.astype(bf16)
    ref[k * frames : (k + 1) * frames] = high
    ref[(count + k) * frames : (count + k + 1) * frames] = (term - high.astype(f32)).astype(bf16)


def head_sums(ref, rows, heads_block, store):
    width = heads_block.shape[0]
    for j in range(ref.shape[1] // width):
        cols = slice(j * width, (j + 1) * width)
        store(cols, dot(ref[:rows, cols], heads_block) + dot(ref[rows:, cols], heads_block))


def same_head(width, head):
    r = lax.broadcasted_iota(jnp.int32, (width, width), 0) // head
    c = lax.broadcasted_iota(jnp.int32, (width, width), 1) // head
    return (r == c).astype(f32).astype(bf16)


def pairs_of(positions):
    return [(c, e) for c in range(positions) for e in range(c + 1)]


def depth_body(
    place_ref, att_ref, emb_ref, codes_ref, gain_ref, w_in_hbm, table_hbm,
    near_hbm, far_hbm, near_twin_hbm, far_twin_hbm, keep_ref, send_ref,
    w_in_ref, table_ref, w_ref, w_out_ref, x_ref, n_ref, n_t_ref, qkv_ref, term_ref, s_ref, p_ref, mix_ref, mix_t_ref, inv_ref,
    logit_ref, g_ref, dr_ref, dqkv_ref, stage_ref, sems, in_sems, table_sem,
    *, weight, head,
):
    frames, positions = codes_ref.shape
    width = x_ref.shape[1]
    entries = table_ref.shape[0]
    dh = w_out_ref.shape[0]
    owners, _, rows_qkv, _ = stage_ref.shape
    rows_out = rows_qkv // 2
    half = width // 2
    tile = 256
    side = place_ref[2]
    z_ref = x_ref
    dz_ref = logit_ref.at[:, :width]
    dmix_ref = logit_ref.at[:, width : width + dh]
    row = lambda c: pl.ds(c * frames, frames)

    tile_cols = lambda j: pl.ds(pl.multiple_of(j * tile, tile), tile)
    load_in = lambda j: pltpu.make_async_copy(
        w_in_hbm.at[:, tile_cols(j)], w_in_ref.at[:, tile_cols(j)], in_sems.at[j]
    )
    load_table = pltpu.make_async_copy(table_hbm, table_ref, table_sem)
    for j in range(width // tile):
        load_in(j).start()
    loads = []
    ring = near_hbm.shape[0]
    quarters = ((0, 0, near_hbm), (0, 1, far_hbm), (1, 0, near_twin_hbm), (1, 1, far_twin_hbm))
    for twin, plane, ref in quarters:
        for back in range(ring):
            at = (place_ref[0] + plane) % 2
            at = at * ring + (place_ref[1] + ring - back) % ring
            at = at * 2 + (side + twin) % 2
            rows = pl.ds(pl.multiple_of(at * rows_qkv, rows_qkv), rows_qkv)
            loads.append(pltpu.make_async_copy(ref.at[back], w_ref.at[rows], sems.at[len(loads)]))
            loads[-1].start()
    load_table.start()
    att = jnp.concatenate([att_ref[h] for h in range(att_ref.shape[0])], axis=1)

    @pl.loop(0, width // tile)
    def _(j):
        cols = pl.ds(pl.multiple_of(j * tile, tile), tile)
        load_in(j).wait()
        hidden = dot(att, w_in_ref[:, cols])
        x_ref[row(0), cols] = hidden
        for c in range(1, positions):
            x_ref[row(c), cols] = hidden + emb_ref[c - 1, :, cols].astype(f32)

    for c in range(positions):
        x = x_ref[row(c), :]
        scale = lax.rsqrt(jnp.mean(x * x, axis=1, keepdims=True) + EPS)
        normed = (x * scale * gain_ref[...]).astype(bf16)
        n_ref[row(c), :] = normed
        n_t_ref[:, row(c)] = normed.T

    for load in loads:
        load.wait()
    for d in range(2 * owners):
        for k in range(2):
            w_out_ref[d * rows_out : (d + 1) * rows_out, k * half : (k + 1) * half] = w_ref[
                d * rows_qkv + k * rows_out : d * rows_qkv + (k + 1) * rows_out, 3 * dh :
            ]

    @pl.loop(0, 3 * dh // tile)
    def _(j):
        cols = pl.ds(pl.multiple_of(j * tile, tile), tile)
        qkv_ref[:, cols] = dot(n_ref[...], w_ref[:, cols]).astype(bf16)

    block = same_head(tile, head)
    scale = 1.0 / math.sqrt(head)
    pairs = pairs_of(positions)
    part = lambda c, k: qkv_ref[row(c), k * dh : (k + 1) * dh].astype(f32)
    count = len(pairs)
    pair = lambda c, e: pl.ds(pairs.index((c, e)) * frames, frames)

    def store_scores(cols, values):
        s_ref[:, cols] = values * scale

    for k, (c, e) in enumerate(pairs):
        put_split(term_ref, k, frames, count, part(c, 0) * part(e, 1))
    head_sums(term_ref, count * frames, block, store_scores)
    for c in range(positions):
        scores = [s_ref[pair(c, e), :] for e in range(c + 1)]
        top = functools.reduce(jnp.maximum, scores)
        raised = [jnp.exp(s - top) for s in scores]
        fraction = 1.0 / functools.reduce(jnp.add, raised)
        mixed = jnp.zeros((frames, dh), f32)
        for e in range(c + 1):
            p = raised[e] * fraction
            p_ref[pair(c, e), :] = p
            mixed = mixed + p * part(e, 2)
        mixed = mixed.astype(bf16)
        mix_ref[row(c), :] = mixed
        mix_t_ref[:, row(c)] = mixed.T

    @pl.loop(0, width // tile)
    def _(j):
        cols = pl.ds(pl.multiple_of(j * tile, tile), tile)
        z_ref[:, cols] = x_ref[:, cols] + dot(mix_ref[...], w_out_ref[:, cols])

    for c in range(positions):
        r = z_ref[row(c), :]
        inv = lax.rsqrt(jnp.mean(r * r, axis=1, keepdims=True) + EPS)
        inv_ref[row(c), :] = jnp.broadcast_to(inv, (frames, inv_ref.shape[1]))
        z = r * inv
        z_ref[row(c), :] = z
        dr_ref[row(c), :] = z.astype(bf16)

    load_table.wait()

    @pl.loop(0, entries // tile)
    def _(j):
        cols = pl.ds(pl.multiple_of(j * tile, tile), tile)
        logit_ref[:, cols] = dot_nt(dr_ref[...], table_ref[cols, :])

    ids = lax.broadcasted_iota(jnp.int32, (frames, entries), 1)
    for c in range(positions):
        s = logit_ref[row(c), :]
        e = jnp.exp(s - jnp.max(s, axis=1, keepdims=True))
        total = jnp.sum(e, axis=1, keepdims=True)
        hit = jnp.where(ids == codes_ref[:, c : c + 1], weight, 0.0)
        g_ref[row(c), :] = (e * (weight / total) - hit).astype(bf16)

    @pl.loop(0, width // tile)
    def _(j):
        cols = pl.ds(pl.multiple_of(j * tile, tile), tile)
        dz_ref[:, cols] = dot(g_ref[...], table_ref[:, cols])

    for c in range(positions):
        dz, z = dz_ref[row(c), :], z_ref[row(c), :]
        along = jnp.mean(dz * z, axis=1, keepdims=True)
        dr_ref[row(c), :] = (inv_ref[row(c), 0:1] * (dz - z * along)).astype(bf16)

    for j in range(width // tile):
        part_out = dot(mix_t_ref[...], dr_ref[:, j * tile : (j + 1) * tile]).astype(bf16)
        stage_ref[:, :, 0:rows_out, :] = part_out.reshape(owners, 2, rows_out, tile)
        k, at = divmod(j * tile, half)
        rows = slice(k * rows_out, (k + 1) * rows_out)
        cols = slice(3 * dh + at, 3 * dh + at + tile)
        keep_ref[:, rows, cols] = stage_ref[:, side, 0:rows_out, :]
        send_ref[:, rows, cols] = stage_ref[:, 1 - side, 0:rows_out, :]

    @pl.loop(0, dh // tile)
    def _(j):
        cols = pl.ds(pl.multiple_of(j * tile, tile), tile)
        dmix_ref[:, cols] = dot_nt(dr_ref[...], w_out_ref[cols, :])

    def store_plain(cols, values):
        s_ref[:, cols] = values

    for k, (c, e) in enumerate(pairs):
        put_split(term_ref, k, frames, count, dmix_ref[row(c), :] * part(e, 2))
    head_sums(term_ref, count * frames, block, store_plain)
    dk = [jnp.zeros((frames, dh), f32) for _ in range(positions)]
    dv = [jnp.zeros((frames, dh), f32) for _ in range(positions)]
    for c in range(positions):
        dm = dmix_ref[row(c), :]
        probs = [p_ref[pair(c, e), :] for e in range(c + 1)]
        dprobs = [s_ref[pair(c, e), :] for e in range(c + 1)]
        along = functools.reduce(jnp.add, [d * p for d, p in zip(dprobs, probs)])
        q = part(c, 0)
        dq = jnp.zeros((frames, dh), f32)
        for e in range(c + 1):
            ds = probs[e] * (dprobs[e] - along) * scale
            dq = dq + ds * part(e, 1)
            dk[e] = dk[e] + ds * q
            dv[e] = dv[e] + probs[e] * dm
        dqkv_ref[row(c), 0:dh] = dq.astype(bf16)
    for c in range(positions):
        dqkv_ref[row(c), dh : 2 * dh] = dk[c].astype(bf16)
        dqkv_ref[row(c), 2 * dh :] = dv[c].astype(bf16)

    @pl.loop(0, 3 * dh // tile)
    def _(j):
        cols = pl.ds(pl.multiple_of(j * tile, tile), tile)
        part_qkv = dot(n_t_ref[...], dqkv_ref[:, cols]).astype(bf16)
        stage_ref[...] = part_qkv.reshape(owners, 2, rows_qkv, tile)
        keep_ref[:, :, cols] = stage_ref[:, side]
        send_ref[:, :, cols] = stage_ref[:, 1 - side]


def pack_body(query_hbm, keys_hbm, values_hbm, o_hbm, in_ref, out_ref, in_sems, out_sems):
    sources = (query_hbm, keys_hbm, values_hbm)
    loads = [pltpu.make_async_copy(s.at[0], in_ref.at[k], in_sems.at[k]) for k, s in enumerate(sources)]
    stores = [
        pltpu.make_async_copy(out_ref.at[:, k], o_hbm.at[:, k], out_sems.at[k]) for k in range(len(sources))
    ]
    for load in loads:
        load.start()
    width = out_ref.shape[3]
    for k in range(len(sources)):
        loads[k].wait()
        for d in range(out_ref.shape[0]):
            out_ref[d, k] = in_ref[k, :, d * width : (d + 1) * width]
        stores[k].start()
    for store in stores:
        store.wait()


def add_cut_body(a_ref, b_ref, o_ref):
    width = o_ref.shape[3]
    for k in range(o_ref.shape[1]):
        cols = slice(k * width, (k + 1) * width)
        o_ref[:, k] = (a_ref[:, :, cols].astype(f32) + b_ref[:, :, cols].astype(f32)).astype(bf16)


def fold_cut_body(x_ref, o_ref):
    width = o_ref.shape[2]
    for j in range(o_ref.shape[0]):
        cols = slice(j * width, (j + 1) * width)
        o_ref[j] = functools.reduce(
            jnp.add, [x_ref[d, :, cols].astype(f32) for d in range(x_ref.shape[0])]
        ).astype(bf16)


def fold_copy_body(x_ref, o_ref):
    total = functools.reduce(jnp.add, [x_ref[d].astype(f32) for d in range(x_ref.shape[0])])
    for j in range(o_ref.shape[0]):
        o_ref[j] = total.astype(bf16)


def lay_out_body(x_ref, qkv_ref, out_ref):
    width = x_ref.shape[2]
    rows_out, cols_out = out_ref.shape
    for j in range(x_ref.shape[0]):
        part, at = x_ref[j].astype(f32), j * width
        if at < qkv_ref.shape[1]:
            qkv_ref[:, at : at + width] = part
        else:
            at -= qkv_ref.shape[1]
            for k in range(2):
                cols = slice(k * (cols_out // 2) + at, k * (cols_out // 2) + at + width)
                out_ref[:, cols] = part[k * rows_out : (k + 1) * rows_out]


VMEM = pl.BlockSpec(memory_space=pltpu.VMEM)
SMEM = pl.BlockSpec(memory_space=pltpu.SMEM)
HBM = pl.BlockSpec(memory_space=pltpu.HBM)


def kernel(body, outs, name, flops, in_specs=None, out_specs=None, scratch=(), room=None):
    many = isinstance(outs, (list, tuple))
    every = list(outs) if many else [outs]
    size = sum(math.prod(o.shape) * o.dtype.itemsize for o in every)

    def call(*args):
        return pl.pallas_call(
            body,
            out_shape=every if many else outs,
            in_specs=in_specs or [VMEM] * len(args),
            out_specs=out_specs or ([VMEM] * len(every) if many else VMEM),
            scratch_shapes=list(scratch),
            cost_estimate=pl.CostEstimate(
                flops=flops,
                bytes_accessed=size + sum(math.prod(a.shape) * a.dtype.itemsize for a in args),
                transcendentals=0,
            ),
            compiler_params=pltpu.CompilerParams(vmem_limit_bytes=room),
            name=name,
        )(*args)

    return call


def shape(dims, dtype=bf16):
    return jax.ShapeDtypeStruct(tuple(dims), dtype)


def to_all(x, axis):
    return lax.all_to_all(x, axis, 0, 0, tiled=True)


def turned(x, axis, k):
    n = lax.axis_size(axis)
    return lax.ppermute(x, axis, [(i, (i + k) % n) for i in range(n)])


def depth_call(weight, place, attended, embedded, codes, gain, w_in, table, weights):
    frames, positions = codes.shape
    width, entries, rows = w_in.shape[1], table.shape[0], frames * positions
    dh = (weights[0].shape[2] - width // 2) // 3
    ring, share, columns = weights[0].shape
    owners = 2 * ring
    cut = shape((owners, share, columns))
    pairs = len(pairs_of(positions)) * frames
    return kernel(
        functools.partial(depth_body, weight=weight, head=DEPTH_HEAD),
        (cut, cut),
        "depth",
        11 * 10**9,
        room=44 << 20,
        in_specs=[SMEM] + [VMEM] * 4 + [HBM] * 6,
        scratch=[
            pltpu.VMEM(w_in.shape, bf16),
            pltpu.VMEM(table.shape, bf16),
            pltpu.VMEM((width, columns), bf16),
            pltpu.VMEM((dh, width), bf16),
            pltpu.VMEM((rows, width), f32),
            pltpu.VMEM((rows, width), bf16),
            pltpu.VMEM((width, rows), bf16),
            pltpu.VMEM((rows, 3 * dh), bf16),
            pltpu.VMEM((2 * pairs, dh), bf16),
            pltpu.VMEM((pairs, dh), f32),
            pltpu.VMEM((pairs, dh), f32),
            pltpu.VMEM((rows, dh), bf16),
            pltpu.VMEM((dh, rows), bf16),
            pltpu.VMEM((rows, 128), f32),
            pltpu.VMEM((rows, entries), f32),
            pltpu.VMEM((rows, entries), bf16),
            pltpu.VMEM((rows, width), bf16),
            pltpu.VMEM((rows, 3 * dh), bf16),
            pltpu.VMEM((owners, 2, share, 256), bf16),
            pltpu.SemaphoreType.DMA((2 * owners,)),
            pltpu.SemaphoreType.DMA((width // 256,)),
            pltpu.SemaphoreType.DMA,
        ],
    )(place, attended, embedded, codes, gain.reshape(1, width), w_in, table, *weights)


def local(query, keys, values, codes, w_in, table, gain, w_qkv, w_out):
    parts = lax.axis_size(CTX)
    frames, positions = codes.shape[1:]
    width, dh = w_in.shape[1], w_out.shape[0] * lax.axis_size(DP)
    entries = table.shape[0]
    place = jnp.stack([lax.axis_index(name) for name in DP])

    blocks = (parts, 3, frames, HEAD_DIM)
    packed = kernel(
        pack_body,
        shape(blocks),
        "pack",
        1 << 20,
        in_specs=[HBM] * 3,
        out_specs=HBM,
        scratch=[
            pltpu.VMEM((3, *query.shape[1:]), bf16),
            pltpu.VMEM(blocks, bf16),
            pltpu.SemaphoreType.DMA((3,)),
            pltpu.SemaphoreType.DMA((3,)),
        ],
    )(query, keys, values)
    w_qkv, w_out, packed = lax.optimization_barrier((w_qkv, w_out, packed))
    both = jnp.concatenate(
        [w_qkv, jnp.concatenate([w_out[:, : width // 2], w_out[:, width // 2 :]], axis=0)], axis=1
    )
    ring = lax.axis_size("dp_1")
    planes = [[w] + [turned(w, "dp_1", k) for k in range(1, ring)] for w in (both, turned(both, "dp_0", 1))]
    weights = [jnp.stack(plane) for plane in planes]
    weights += [turned(w, "dp_2", 1) for w in weights]

    moved = to_all(packed, CTX)
    embedded = kernel(
        embed_body,
        shape((positions - 1, frames, width)),
        "embed",
        2 * (positions - 1) * frames * entries * width,
        room=10 << 20,
        scratch=[pltpu.VMEM(((positions - 1) * frames, entries), bf16)],
    )(codes[0], table)

    heads = kernel(
        functools.partial(attend_body, step=2),
        shape((parts, frames, HEAD_DIM)),
        "attend",
        4 * (parts * frames) ** 2 * HEAD_DIM,
        room=24 << 20,
    )(moved)
    attended = to_all(heads, CTX)

    keep, send = depth_call(
        1.0 / lax.axis_size(DP), place, attended, embedded, codes[0], gain, w_in, table, weights
    )
    swapped = turned(send, "dp_2", 1)
    owners, rows, columns = keep.shape
    planes, lane = lax.axis_size("ctx_0"), columns // parts
    halves = shape((owners, planes, rows, columns // planes))
    chip_sum = kernel(add_cut_body, halves, "chip_sum", 1 << 22, room=16 << 20)(keep, swapped)
    chip_sum = chip_sum.reshape(owners * planes, rows, columns // planes)
    plane_sum = kernel(
        fold_cut_body, shape((parts // planes, rows, lane)), "plane_sum", 1 << 22, room=8 << 20
    )(to_all(chip_sum, PLANE))
    whole_sum = kernel(fold_copy_body, shape((parts, rows, lane)), "whole_sum", 1 << 20, room=4 << 20)(
        to_all(plane_sum, "ctx_1")
    )
    return kernel(
        lay_out_body, (shape(w_qkv.shape, f32), shape(w_out.shape, f32)), "lay_out", 1 << 20, room=4 << 20
    )(to_all(whole_sum, CTX))


def solution(mesh):
    torus = Mesh(mesh.devices.reshape(2, 4, 2, 2, 8), DP + CTX)
    frames = P(DP, CTX, None)
    in_specs = (frames, frames, frames, frames, P(), P(), P(), P(DP, None), P(DP, None))
    out_specs = (P(DP, None), P(DP, None))
    return jax.shard_map(local, mesh=torus, in_specs=in_specs, out_specs=out_specs, check_vma=False)
```

```python
import functools
import math

import jax
import jax.numpy as jnp
from jax import lax
from jax.experimental import pallas as pl
from jax.experimental.pallas import tpu as pltpu
from jax.sharding import Mesh
from jax.sharding import PartitionSpec as P

HEAD_DIM = 128
DEPTH_HEAD = 64
DP = ("dp_0", "dp_1", "dp_2")
CTX = ("ctx_0", "ctx_1")
PLANE = ("dp_0", "dp_1", "ctx_0")

bf16, f32 = jnp.bfloat16, jnp.float32
NEG = -1e30
EPS = 1e-6
NT = (((1,), (1,)), ((), ()))


def dot(a, b):
    return jnp.dot(a, b, preferred_element_type=f32)


def dot_nt(a, b):
    return lax.dot_general(a, b, NT, preferred_element_type=f32)


def attend_body(x_ref, o_ref, *, step):
    blocks, _, rows, dim = x_ref.shape
    for i in range(0, blocks, step):
        seen = i + step
        q = x_ref[i:seen, 0].reshape(step * rows, dim)
        k = x_ref[0:seen, 1].reshape(seen * rows, dim)
        v = x_ref[0:seen, 2].reshape(seen * rows, dim)
        s = dot_nt(q, k)
        shape = (step * rows, step * rows)
        ok = lax.broadcasted_iota(jnp.int32, shape, 1) <= lax.broadcasted_iota(jnp.int32, shape, 0)
        last = jnp.where(ok, s[:, i * rows :], NEG)
        s = last if i == 0 else jnp.concatenate([s[:, : i * rows], last], axis=1)
        p = jnp.exp2((s - jnp.max(s, axis=1, keepdims=True)) * (math.log2(math.e) / math.sqrt(dim)))
        total = jnp.sum(p, axis=1, keepdims=True)
        out = dot(p.astype(bf16), v) / total
        o_ref[i:seen] = out.astype(bf16).reshape(step, rows, dim)


def embed_body(codes_ref, table_ref, o_ref, hot_ref):
    count, frames, width = o_ref.shape
    entries = table_ref.shape[0]
    ids = lax.broadcasted_iota(jnp.int32, (frames, entries), 1)
    for c in range(count):
        hot_ref[c * frames : (c + 1) * frames] = (
            (ids == codes_ref[:, c : c + 1]).astype(f32).astype(bf16)
        )
    tile = 256

    @pl.loop(0, width // tile)
    def _(j):
        cols = pl.ds(pl.multiple_of(j * tile, tile), tile)
        rows = dot(hot_ref[...], table_ref[:, cols])
        o_ref[:, :, cols] = rows.astype(bf16).reshape(count, frames, tile)


def put_split(ref, rows, term, width):
    high = term.astype(bf16)
    low = (term - high.astype(f32)).astype(bf16)
    for j in range(term.shape[1] // width):
        cols = slice(j * width, (j + 1) * width)
        ref[rows, 2 * j * width : (2 * j + 1) * width] = high[:, cols]
        ref[rows, (2 * j + 1) * width : (2 * j + 2) * width] = low[:, cols]


def head_sums(ref, heads_block, store):
    depth, width = heads_block.shape
    for j in range(ref.shape[1] // depth):
        store(
            slice(j * width, (j + 1) * width),
            dot(ref[:, j * depth : (j + 1) * depth], heads_block),
        )


def same_head(width, head):
    r = lax.broadcasted_iota(jnp.int32, (width, width), 0) // head
    c = lax.broadcasted_iota(jnp.int32, (width, width), 1) // head
    return (r == c).astype(f32).astype(bf16)


def pairs_of(positions):
    return [(c, e) for c in range(positions) for e in range(c + 1)]


def depth_body(*refs, weight, head):
    place_ref, att_ref, codes_ref, gain_ref, emb_hbm, w_in_hbm, table_hbm = refs[:7]
    shards = refs[7:-26]
    keep_ref, send_ref, emb_ref, w_in_ref, table_ref, w_ref, w_out_ref, x_ref, n_ref = refs[-26:-17]
    n_t_ref, qkv_ref, term_ref, s_ref, p_ref, mix_ref, mix_t_ref, inv_ref = refs[-17:-9]
    logit_ref, g_ref, dr_ref, dqkv_ref, stage_ref, sems, in_sems, emb_sem, table_sem = refs[-9:]
    frames, positions = codes_ref.shape
    width = x_ref.shape[1]
    entries = table_ref.shape[0]
    dh = w_out_ref.shape[0]
    owners, _, rows_qkv, _ = stage_ref.shape
    rows_out = rows_qkv // 2
    half = width // 2
    tile = 256
    side = place_ref[2]
    z_ref = x_ref
    dz_ref = logit_ref.at[:, :width]
    dmix_ref = logit_ref.at[:, width : width + dh]
    row = lambda c: pl.ds(c * frames, frames)

    tile_cols = lambda j: pl.ds(pl.multiple_of(j * tile, tile), tile)
    load_in = lambda j: pltpu.make_async_copy(
        w_in_hbm.at[:, tile_cols(j)], w_in_ref.at[:, tile_cols(j)], in_sems.at[j]
    )
    load_emb = pltpu.make_async_copy(emb_hbm, emb_ref, emb_sem)
    load_table = pltpu.make_async_copy(table_hbm, table_ref, table_sem)
    load_in(0).start()
    load_emb.start()
    for j in range(1, width // tile):
        load_in(j).start()
    loads = []
    ring = len(shards) // 4
    for k, ref in enumerate(shards):
        twin, plane, back = k // (2 * ring), k // ring % 2, k % ring
        at = (place_ref[0] + plane) % 2
        at = at * ring + (place_ref[1] + ring - back) % ring
        at = at * 2 + (side + twin) % 2
        rows = pl.ds(pl.multiple_of(at * rows_qkv, rows_qkv), rows_qkv)
        loads.append(pltpu.make_async_copy(ref, w_ref.at[rows], sems.at[k]))
        loads[-1].start()
    load_table.start()
    load_emb.wait()
    att = jnp.concatenate([att_ref[h] for h in range(att_ref.shape[0])], axis=1)

    @pl.loop(0, width // tile)
    def _(j):
        cols = pl.ds(pl.multiple_of(j * tile, tile), tile)
        load_in(j).wait()
        hidden = dot(att, w_in_ref[:, cols])
        x_ref[row(0), cols] = hidden
        for c in range(1, positions):
            x_ref[row(c), cols] = hidden + emb_ref[c - 1, :, cols].astype(f32)

    for c in range(positions):
        x = x_ref[row(c), :]
        scale = lax.rsqrt(jnp.mean(x * x, axis=1, keepdims=True) + EPS)
        normed = (x * scale * gain_ref[...]).astype(bf16)
        n_ref[row(c), :] = normed
        n_t_ref[:, row(c)] = normed.T

    for load in loads:
        load.wait()
    for d in range(2 * owners):
        for k in range(2):
            w_out_ref[d * rows_out : (d + 1) * rows_out, k * half : (k + 1) * half] = w_ref[
                d * rows_qkv + k * rows_out : d * rows_qkv + (k + 1) * rows_out, 3 * dh :
            ]

    @pl.loop(0, 3 * dh // tile)
    def _(j):
        cols = pl.ds(pl.multiple_of(j * tile, tile), tile)
        qkv_ref[:, cols] = dot(n_ref[...], w_ref[:, cols]).astype(bf16)

    block = jnp.concatenate([same_head(tile, head)] * 2, axis=0)
    scale = 1.0 / math.sqrt(head)
    pairs = pairs_of(positions)
    part = lambda c, k: qkv_ref[row(c), k * dh : (k + 1) * dh].astype(f32)
    pair = lambda c, e: pl.ds(pairs.index((c, e)) * frames, frames)

    def store_scores(cols, values):
        s_ref[:, cols] = values * scale

    for c, e in pairs:
        put_split(term_ref, pair(c, e), part(c, 0) * part(e, 1), tile)
    head_sums(term_ref, block, store_scores)
    for c in range(positions):
        scores = [s_ref[pair(c, e), :] for e in range(c + 1)]
        top = functools.reduce(jnp.maximum, scores)
        raised = [jnp.exp(s - top) for s in scores]
        fraction = 1.0 / functools.reduce(jnp.add, raised)
        mixed = jnp.zeros((frames, dh), f32)
        for e in range(c + 1):
            p = raised[e] * fraction
            p_ref[pair(c, e), :] = p
            mixed = mixed + p * part(e, 2)
        mixed = mixed.astype(bf16)
        mix_ref[row(c), :] = mixed
        mix_t_ref[:, row(c)] = mixed.T

    @pl.loop(0, width // tile)
    def _(j):
        cols = pl.ds(pl.multiple_of(j * tile, tile), tile)
        z_ref[:, cols] = x_ref[:, cols] + dot(mix_ref[...], w_out_ref[:, cols])

    for c in range(positions):
        r = z_ref[row(c), :]
        inv = lax.rsqrt(jnp.mean(r * r, axis=1, keepdims=True) + EPS)
        inv_ref[row(c), :] = jnp.broadcast_to(inv, (frames, inv_ref.shape[1]))
        z = r * inv
        z_ref[row(c), :] = z
        dr_ref[row(c), :] = z.astype(bf16)

    load_table.wait()

    @pl.loop(0, entries // tile)
    def _(j):
        cols = pl.ds(pl.multiple_of(j * tile, tile), tile)
        logit_ref[:, cols] = dot_nt(dr_ref[...], table_ref[cols, :])

    ids = lax.broadcasted_iota(jnp.int32, (frames, entries), 1)
    for c in range(positions):
        s = logit_ref[row(c), :]
        e = jnp.exp(s - jnp.max(s, axis=1, keepdims=True))
        total = jnp.sum(e, axis=1, keepdims=True)
        hit = jnp.where(ids == codes_ref[:, c : c + 1], weight, 0.0)
        g_ref[row(c), :] = (e * (weight / total) - hit).astype(bf16)

    @pl.loop(0, width // tile)
    def _(j):
        cols = pl.ds(pl.multiple_of(j * tile, tile), tile)
        dz_ref[:, cols] = dot(g_ref[...], table_ref[:, cols])

    for c in range(positions):
        dz, z = dz_ref[row(c), :], z_ref[row(c), :]
        along = jnp.mean(dz * z, axis=1, keepdims=True)
        dr_ref[row(c), :] = (inv_ref[row(c), 0:1] * (dz - z * along)).astype(bf16)

    for j in range(width // tile):
        part_out = dot(mix_t_ref[...], dr_ref[:, j * tile : (j + 1) * tile]).astype(bf16)
        stage_ref[:, :, 0:rows_out, :] = part_out.reshape(owners, 2, rows_out, tile)
        k, at = divmod(j * tile, half)
        rows = slice(k * rows_out, (k + 1) * rows_out)
        cols = slice(3 * dh + at, 3 * dh + at + tile)
        keep_ref[:, rows, cols] = stage_ref[:, side, 0:rows_out, :]
        send_ref[:, rows, cols] = stage_ref[:, 1 - side, 0:rows_out, :]

    @pl.loop(0, dh // tile)
    def _(j):
        cols = pl.ds(pl.multiple_of(j * tile, tile), tile)
        dmix_ref[:, cols] = dot_nt(dr_ref[...], w_out_ref[cols, :])

    def store_plain(cols, values):
        s_ref[:, cols] = values

    for c, e in pairs:
        put_split(term_ref, pair(c, e), dmix_ref[row(c), :] * part(e, 2), tile)
    head_sums(term_ref, block, store_plain)
    dk = [jnp.zeros((frames, dh), f32) for _ in range(positions)]
    dv = [jnp.zeros((frames, dh), f32) for _ in range(positions)]
    for c in range(positions):
        dm = dmix_ref[row(c), :]
        probs = [p_ref[pair(c, e), :] for e in range(c + 1)]
        dprobs = [s_ref[pair(c, e), :] for e in range(c + 1)]
        along = functools.reduce(jnp.add, [d * p for d, p in zip(dprobs, probs)])
        q = part(c, 0)
        dq = jnp.zeros((frames, dh), f32)
        for e in range(c + 1):
            ds = probs[e] * (dprobs[e] - along) * scale
            dq = dq + ds * part(e, 1)
            dk[e] = dk[e] + ds * q
            dv[e] = dv[e] + probs[e] * dm
        dqkv_ref[row(c), 0:dh] = dq.astype(bf16)
    for c in range(positions):
        dqkv_ref[row(c), dh : 2 * dh] = dk[c].astype(bf16)
        dqkv_ref[row(c), 2 * dh :] = dv[c].astype(bf16)

    @pl.loop(0, 3 * dh // tile)
    def _(j):
        cols = pl.ds(pl.multiple_of(j * tile, tile), tile)
        part_qkv = dot(n_t_ref[...], dqkv_ref[:, cols]).astype(bf16)
        stage_ref[...] = part_qkv.reshape(owners, 2, rows_qkv, tile)
        keep_ref[:, :, cols] = stage_ref[:, side]
        send_ref[:, :, cols] = stage_ref[:, 1 - side]


def pack_body(query_hbm, keys_hbm, values_hbm, o_hbm, in_ref, out_ref, in_sems, out_sems):
    sources = (query_hbm, keys_hbm, values_hbm)
    loads = [pltpu.make_async_copy(s.at[0], in_ref.at[k], in_sems.at[k]) for k, s in enumerate(sources)]
    stores = [
        pltpu.make_async_copy(out_ref.at[:, k], o_hbm.at[:, k], out_sems.at[k]) for k in range(len(sources))
    ]
    for load in loads:
        load.start()
    width = out_ref.shape[3]
    for k in range(len(sources)):
        loads[k].wait()
        for d in range(out_ref.shape[0]):
            out_ref[d, k] = in_ref[k, :, d * width : (d + 1) * width]
        stores[k].start()
    for store in stores:
        store.wait()


def add_cut_body(a_ref, b_ref, o_ref):
    width = o_ref.shape[3]
    for k in range(o_ref.shape[1]):
        cols = slice(k * width, (k + 1) * width)
        o_ref[:, k] = (a_ref[:, :, cols].astype(f32) + b_ref[:, :, cols].astype(f32)).astype(bf16)


def fold_cut_body(x_ref, o_ref):
    width = o_ref.shape[2]
    for j in range(o_ref.shape[0]):
        cols = slice(j * width, (j + 1) * width)
        o_ref[j] = functools.reduce(
            jnp.add, [x_ref[d, :, cols].astype(f32) for d in range(x_ref.shape[0])]
        ).astype(bf16)


def fold_copy_body(x_ref, o_ref):
    total = functools.reduce(jnp.add, [x_ref[d].astype(f32) for d in range(x_ref.shape[0])])
    for j in range(o_ref.shape[0]):
        o_ref[j] = total.astype(bf16)


def lay_out_body(x_ref, qkv_ref, out_ref):
    width = x_ref.shape[2]
    rows_out, cols_out = out_ref.shape
    for j in range(x_ref.shape[0]):
        part, at = x_ref[j].astype(f32), j * width
        if at < qkv_ref.shape[1]:
            qkv_ref[:, at : at + width] = part
        else:
            at -= qkv_ref.shape[1]
            for k in range(2):
                cols = slice(k * (cols_out // 2) + at, k * (cols_out // 2) + at + width)
                out_ref[:, cols] = part[k * rows_out : (k + 1) * rows_out]


VMEM = pl.BlockSpec(memory_space=pltpu.VMEM)
SMEM = pl.BlockSpec(memory_space=pltpu.SMEM)
HBM = pl.BlockSpec(memory_space=pltpu.HBM)


def kernel(body, outs, name, flops, in_specs=None, out_specs=None, scratch=(), room=None):
    many = isinstance(outs, (list, tuple))
    every = list(outs) if many else [outs]
    size = sum(math.prod(o.shape) * o.dtype.itemsize for o in every)

    def call(*args):
        return pl.pallas_call(
            body,
            out_shape=every if many else outs,
            in_specs=in_specs or [VMEM] * len(args),
            out_specs=out_specs or ([VMEM] * len(every) if many else VMEM),
            scratch_shapes=list(scratch),
            cost_estimate=pl.CostEstimate(
                flops=flops,
                bytes_accessed=size + sum(math.prod(a.shape) * a.dtype.itemsize for a in args),
                transcendentals=0,
            ),
            compiler_params=pltpu.CompilerParams(vmem_limit_bytes=room),
            name=name,
        )(*args)

    return call


def shape(dims, dtype=bf16):
    return jax.ShapeDtypeStruct(tuple(dims), dtype)


def to_all(x, axis):
    return lax.all_to_all(x, axis, 0, 0, tiled=True)


def turned(x, axis, k):
    n = lax.axis_size(axis)
    return lax.ppermute(x, axis, [(i, (i + k) % n) for i in range(n)])


def depth_call(weight, place, attended, embedded, codes, gain, w_in, table, weights):
    frames, positions = codes.shape
    width, entries, rows = w_in.shape[1], table.shape[0], frames * positions
    dh = (weights[0].shape[1] - width // 2) // 3
    share, columns = weights[0].shape
    owners = len(weights) // 2
    cut = shape((owners, share, columns))
    pairs = len(pairs_of(positions)) * frames
    return kernel(
        functools.partial(depth_body, weight=weight, head=DEPTH_HEAD),
        (cut, cut),
        "depth",
        11 * 10**9,
        room=42 << 20,
        in_specs=[SMEM] + [VMEM] * 3 + [HBM] * (3 + len(weights)),
        scratch=[
            pltpu.VMEM(embedded.shape, bf16),
            pltpu.VMEM(w_in.shape, bf16),
            pltpu.VMEM(table.shape, bf16),
            pltpu.VMEM((width, columns), bf16),
            pltpu.VMEM((dh, width), bf16),
            pltpu.VMEM((rows, width), f32),
            pltpu.VMEM((rows, width), bf16),
            pltpu.VMEM((width, rows), bf16),
            pltpu.VMEM((rows, 3 * dh), bf16),
            pltpu.VMEM((pairs, 2 * dh), bf16),
            pltpu.VMEM((pairs, dh), f32),
            pltpu.VMEM((pairs, dh), f32),
            pltpu.VMEM((rows, dh), bf16),
            pltpu.VMEM((dh, rows), bf16),
            pltpu.VMEM((rows, 128), f32),
            pltpu.VMEM((rows, entries), f32),
            pltpu.VMEM((rows, entries), bf16),
            pltpu.VMEM((rows, width), bf16),
            pltpu.VMEM((rows, 3 * dh), bf16),
            pltpu.VMEM((owners, 2, share, 256), bf16),
            pltpu.SemaphoreType.DMA((2 * owners,)),
            pltpu.SemaphoreType.DMA((width // 256,)),
            pltpu.SemaphoreType.DMA,
            pltpu.SemaphoreType.DMA,
        ],
    )(place, attended, codes, gain.reshape(1, width), embedded, w_in, table, *weights)


def local(query, keys, values, codes, w_in, table, gain, w_qkv, w_out):
    parts = lax.axis_size(CTX)
    frames, positions = codes.shape[1:]
    width, dh = w_in.shape[1], w_out.shape[0] * lax.axis_size(DP)
    entries = table.shape[0]
    place = jnp.stack([lax.axis_index(name) for name in DP])

    blocks = (parts, 3, frames, HEAD_DIM)
    packed = kernel(
        pack_body,
        shape(blocks),
        "pack",
        1 << 20,
        in_specs=[HBM] * 3,
        out_specs=HBM,
        scratch=[
            pltpu.VMEM((3, *query.shape[1:]), bf16),
            pltpu.VMEM(blocks, bf16),
            pltpu.SemaphoreType.DMA((3,)),
            pltpu.SemaphoreType.DMA((3,)),
        ],
    )(query, keys, values)
    w_qkv, w_out, packed = lax.optimization_barrier((w_qkv, w_out, packed))
    both = jnp.concatenate(
        [w_qkv, jnp.concatenate([w_out[:, : width // 2], w_out[:, width // 2 :]], axis=0)], axis=1
    )
    embedded = kernel(
        embed_body,
        shape((positions - 1, frames, width)),
        "embed",
        2 * (positions - 1) * frames * entries * width,
        room=10 << 20,
        scratch=[pltpu.VMEM(((positions - 1) * frames, entries), bf16)],
    )(codes[0], table)
    other, embedded = lax.optimization_barrier((turned(both, "dp_0", 1), embedded))
    ring = lax.axis_size("dp_1")
    weights = [w if k == 0 else turned(w, "dp_1", k) for w in (both, other) for k in range(ring)]
    weights += [turned(w, "dp_2", 1) for w in weights]

    moved = to_all(packed, CTX)
    moved, embedded, weights, place = lax.optimization_barrier((moved, embedded, weights, place))

    heads = kernel(
        functools.partial(attend_body, step=2),
        shape((parts, frames, HEAD_DIM)),
        "attend",
        4 * (parts * frames) ** 2 * HEAD_DIM,
        room=24 << 20,
    )(moved)
    attended = to_all(heads, CTX)

    keep, send = depth_call(
        1.0 / lax.axis_size(DP), place, attended, embedded, codes[0], gain, w_in, table, weights
    )
    swapped = turned(send, "dp_2", 1)
    owners, rows, columns = keep.shape
    planes, lane = lax.axis_size("ctx_0"), columns // parts
    halves = shape((owners, planes, rows, columns // planes))
    chip_sum = kernel(add_cut_body, halves, "chip_sum", 1 << 22, room=16 << 20)(keep, swapped)
    chip_sum = chip_sum.reshape(owners * planes, rows, columns // planes)
    plane_sum = kernel(
        fold_cut_body, shape((parts // planes, rows, lane)), "plane_sum", 1 << 22, room=8 << 20
    )(to_all(chip_sum, PLANE))
    whole_sum = kernel(fold_copy_body, shape((parts, rows, lane)), "whole_sum", 1 << 20, room=4 << 20)(
        to_all(plane_sum, "ctx_1")
    )
    return kernel(
        lay_out_body, (shape(w_qkv.shape, f32), shape(w_out.shape, f32)), "lay_out", 1 << 20, room=4 << 20
    )(to_all(whole_sum, CTX))


def solution(mesh):
    torus = Mesh(mesh.devices.reshape(2, 4, 2, 2, 8), DP + CTX)
    frames = P(DP, CTX, None)
    in_specs = (frames, frames, frames, frames, P(), P(), P(), P(DP, None), P(DP, None))
    out_specs = (P(DP, None), P(DP, None))
    return jax.shard_map(local, mesh=torus, in_specs=in_specs, out_specs=out_specs, check_vma=False)
```

```python
import functools
import math

import jax
import jax.numpy as jnp
from jax import lax
from jax.experimental import pallas as pl
from jax.experimental.pallas import tpu as pltpu
from jax.sharding import Mesh
from jax.sharding import PartitionSpec as P

HEAD_DIM = 128
DEPTH_HEAD = 64
DP = ("dp_0", "dp_1", "dp_2")
CTX = ("ctx_0", "ctx_1")
PLANE = ("dp_0", "dp_1", "ctx_0")

bf16, f32 = jnp.bfloat16, jnp.float32
NEG = -1e30
EPS = 1e-6
NT = (((1,), (1,)), ((), ()))


def dot(a, b):
    return jnp.dot(a, b, preferred_element_type=f32)


def dot_nt(a, b):
    return lax.dot_general(a, b, NT, preferred_element_type=f32)


def attend_body(x_ref, o_ref, *, step):
    blocks, _, rows, dim = x_ref.shape
    for i in range(0, blocks, step):
        seen = i + step
        q = x_ref[i:seen, 0].reshape(step * rows, dim)
        k = x_ref[0:seen, 1].reshape(seen * rows, dim)
        v = x_ref[0:seen, 2].reshape(seen * rows, dim)
        s = dot_nt(q, k)
        shape = (step * rows, step * rows)
        ok = lax.broadcasted_iota(jnp.int32, shape, 1) <= lax.broadcasted_iota(jnp.int32, shape, 0)
        last = jnp.where(ok, s[:, i * rows :], NEG)
        s = last if i == 0 else jnp.concatenate([s[:, : i * rows], last], axis=1)
        p = jnp.exp2((s - jnp.max(s, axis=1, keepdims=True)) * (math.log2(math.e) / math.sqrt(dim)))
        total = jnp.sum(p, axis=1, keepdims=True)
        out = dot(p.astype(bf16), v) / total
        o_ref[i:seen] = out.astype(bf16).reshape(step, rows, dim)


def embed_body(codes_ref, table_ref, o_ref, hot_ref):
    count, frames, width = o_ref.shape
    entries = table_ref.shape[0]
    ids = lax.broadcasted_iota(jnp.int32, (frames, entries), 1)
    for c in range(count):
        hot_ref[c * frames : (c + 1) * frames] = (
            (ids == codes_ref[:, c : c + 1]).astype(f32).astype(bf16)
        )
    tile = 256

    @pl.loop(0, width // tile)
    def _(j):
        cols = pl.ds(pl.multiple_of(j * tile, tile), tile)
        rows = dot(hot_ref[...], table_ref[:, cols])
        o_ref[:, :, cols] = rows.astype(bf16).reshape(count, frames, tile)


def put_split(ref, rows, term, width):
    high = term.astype(bf16)
    low = (term - high.astype(f32)).astype(bf16)
    for j in range(term.shape[1] // width):
        cols = slice(j * width, (j + 1) * width)
        ref[rows, 2 * j * width : (2 * j + 1) * width] = high[:, cols]
        ref[rows, (2 * j + 1) * width : (2 * j + 2) * width] = low[:, cols]


def head_sums(ref, heads_block, store):
    depth, width = heads_block.shape
    for j in range(ref.shape[1] // depth):
        store(
            slice(j * width, (j + 1) * width),
            dot(ref[:, j * depth : (j + 1) * depth], heads_block),
        )


def same_head(width, head):
    r = lax.broadcasted_iota(jnp.int32, (width, width), 0) // head
    c = lax.broadcasted_iota(jnp.int32, (width, width), 1) // head
    return (r == c).astype(f32).astype(bf16)


def pairs_of(positions):
    return [(c, e) for c in range(positions) for e in range(c + 1)]


def depth_body(*refs, weight, head):
    place_ref, att_ref, codes_ref, gain_ref, emb_hbm, w_in_hbm, table_hbm = refs[:7]
    shards = refs[7:-26]
    keep_ref, send_ref, emb_ref, w_in_ref, table_ref, w_ref, w_out_ref, x_ref, n_ref = refs[-26:-17]
    n_t_ref, qkv_ref, term_ref, s_ref, p_ref, mix_ref, mix_t_ref, inv_ref = refs[-17:-9]
    logit_ref, g_ref, dr_ref, dqkv_ref, stage_ref, sems, in_sems, emb_sem, table_sem = refs[-9:]
    frames, positions = codes_ref.shape
    width = x_ref.shape[1]
    entries = table_ref.shape[0]
    dh = w_out_ref.shape[0]
    owners, _, rows_qkv, _ = stage_ref.shape
    rows_out = rows_qkv // 2
    half = width // 2
    tile = 256
    side = place_ref[2]
    z_ref = x_ref
    dz_ref = logit_ref.at[:, :width]
    dmix_ref = logit_ref.at[:, width : width + dh]
    row = lambda c: pl.ds(c * frames, frames)

    tile_cols = lambda j: pl.ds(pl.multiple_of(j * tile, tile), tile)
    load_in = lambda j: pltpu.make_async_copy(
        w_in_hbm.at[:, tile_cols(j)], w_in_ref.at[:, tile_cols(j)], in_sems.at[j]
    )
    load_emb = pltpu.make_async_copy(emb_hbm, emb_ref, emb_sem)
    load_table = pltpu.make_async_copy(table_hbm, table_ref, table_sem)
    load_in(0).start()
    load_emb.start()
    for j in range(1, width // tile):
        load_in(j).start()
    loads = []
    ring = len(shards) // 4
    for k, ref in enumerate(shards):
        twin, plane, back = k // (2 * ring), k // ring % 2, k % ring
        at = (place_ref[0] + plane) % 2
        at = at * ring + (place_ref[1] + ring - back) % ring
        at = at * 2 + (side + twin) % 2
        rows = pl.ds(pl.multiple_of(at * rows_qkv, rows_qkv), rows_qkv)
        loads.append(pltpu.make_async_copy(ref, w_ref.at[rows], sems.at[k]))
    load_emb.wait()
    for j in range(width // tile):
        load_in(j).wait()
    for load in loads:
        load.start()
    att = jnp.concatenate([att_ref[h] for h in range(att_ref.shape[0])], axis=1)

    @pl.loop(0, width // tile, unroll=4)
    def _(j):
        cols = pl.ds(pl.multiple_of(j * tile, tile), tile)
        hidden = dot(att, w_in_ref[:, cols])
        x_ref[row(0), cols] = hidden
        for c in range(1, positions):
            x_ref[row(c), cols] = hidden + emb_ref[c - 1, :, cols].astype(f32)

    for c in range(positions):
        x = x_ref[row(c), :]
        scale = lax.rsqrt(jnp.mean(x * x, axis=1, keepdims=True) + EPS)
        normed = (x * scale * gain_ref[...]).astype(bf16)
        n_ref[row(c), :] = normed
        n_t_ref[:, row(c)] = normed.T

    for load in loads:
        load.wait()
    load_table.start()
    for d in range(2 * owners):
        for k in range(2):
            w_out_ref[d * rows_out : (d + 1) * rows_out, k * half : (k + 1) * half] = w_ref[
                d * rows_qkv + k * rows_out : d * rows_qkv + (k + 1) * rows_out, 3 * dh :
            ]

    @pl.loop(0, 3 * dh // tile, unroll=6)
    def _(j):
        cols = pl.ds(pl.multiple_of(j * tile, tile), tile)
        qkv_ref[:, cols] = dot(n_ref[...], w_ref[:, cols]).astype(bf16)

    block = jnp.concatenate([same_head(tile, head)] * 2, axis=0)
    scale = 1.0 / math.sqrt(head)
    pairs = pairs_of(positions)
    part = lambda c, k: qkv_ref[row(c), k * dh : (k + 1) * dh].astype(f32)
    pair = lambda c, e: pl.ds(pairs.index((c, e)) * frames, frames)

    def store_scores(cols, values):
        s_ref[:, cols] = values * scale

    for c, e in pairs:
        put_split(term_ref, pair(c, e), part(c, 0) * part(e, 1), tile)
    head_sums(term_ref, block, store_scores)
    for c in range(positions):
        scores = [s_ref[pair(c, e), :] for e in range(c + 1)]
        top = functools.reduce(jnp.maximum, scores)
        raised = [jnp.exp(s - top) for s in scores]
        fraction = 1.0 / functools.reduce(jnp.add, raised)
        mixed = jnp.zeros((frames, dh), f32)
        for e in range(c + 1):
            p = raised[e] * fraction
            p_ref[pair(c, e), :] = p
            mixed = mixed + p * part(e, 2)
        mixed = mixed.astype(bf16)
        mix_ref[row(c), :] = mixed
        mix_t_ref[:, row(c)] = mixed.T

    @pl.loop(0, width // tile, unroll=4)
    def _(j):
        cols = pl.ds(pl.multiple_of(j * tile, tile), tile)
        z_ref[:, cols] = x_ref[:, cols] + dot(mix_ref[...], w_out_ref[:, cols])

    for c in range(positions):
        r = z_ref[row(c), :]
        inv = lax.rsqrt(jnp.mean(r * r, axis=1, keepdims=True) + EPS)
        inv_ref[row(c), :] = jnp.broadcast_to(inv, (frames, inv_ref.shape[1]))
        z = r * inv
        z_ref[row(c), :] = z
        dr_ref[row(c), :] = z.astype(bf16)

    load_table.wait()

    @pl.loop(0, entries // tile, unroll=8)
    def _(j):
        cols = pl.ds(pl.multiple_of(j * tile, tile), tile)
        logit_ref[:, cols] = dot_nt(dr_ref[...], table_ref[cols, :])

    ids = lax.broadcasted_iota(jnp.int32, (frames, entries), 1)
    for c in range(positions):
        s = logit_ref[row(c), :]
        e = jnp.exp(s - jnp.max(s, axis=1, keepdims=True))
        total = jnp.sum(e, axis=1, keepdims=True)
        hit = jnp.where(ids == codes_ref[:, c : c + 1], weight, 0.0)
        g_ref[row(c), :] = (e * (weight / total) - hit).astype(bf16)

    @pl.loop(0, width // tile, unroll=4)
    def _(j):
        cols = pl.ds(pl.multiple_of(j * tile, tile), tile)
        dz_ref[:, cols] = dot(g_ref[...], table_ref[:, cols])

    for c in range(positions):
        dz, z = dz_ref[row(c), :], z_ref[row(c), :]
        along = jnp.mean(dz * z, axis=1, keepdims=True)
        dr_ref[row(c), :] = (inv_ref[row(c), 0:1] * (dz - z * along)).astype(bf16)

    for j in range(width // tile):
        part_out = dot(mix_t_ref[...], dr_ref[:, j * tile : (j + 1) * tile]).astype(bf16)
        stage_ref[:, :, 0:rows_out, :] = part_out.reshape(owners, 2, rows_out, tile)
        k, at = divmod(j * tile, half)
        rows = slice(k * rows_out, (k + 1) * rows_out)
        cols = slice(3 * dh + at, 3 * dh + at + tile)
        keep_ref[:, rows, cols] = stage_ref[:, side, 0:rows_out, :]
        send_ref[:, rows, cols] = stage_ref[:, 1 - side, 0:rows_out, :]

    @pl.loop(0, dh // tile, unroll=2)
    def _(j):
        cols = pl.ds(pl.multiple_of(j * tile, tile), tile)
        dmix_ref[:, cols] = dot_nt(dr_ref[...], w_out_ref[cols, :])

    def store_plain(cols, values):
        s_ref[:, cols] = values

    for c, e in pairs:
        put_split(term_ref, pair(c, e), dmix_ref[row(c), :] * part(e, 2), tile)
    head_sums(term_ref, block, store_plain)
    dk = [jnp.zeros((frames, dh), f32) for _ in range(positions)]
    dv = [jnp.zeros((frames, dh), f32) for _ in range(positions)]
    for c in range(positions):
        dm = dmix_ref[row(c), :]
        probs = [p_ref[pair(c, e), :] for e in range(c + 1)]
        dprobs = [s_ref[pair(c, e), :] for e in range(c + 1)]
        along = functools.reduce(jnp.add, [d * p for d, p in zip(dprobs, probs)])
        q = part(c, 0)
        dq = jnp.zeros((frames, dh), f32)
        for e in range(c + 1):
            ds = probs[e] * (dprobs[e] - along) * scale
            dq = dq + ds * part(e, 1)
            dk[e] = dk[e] + ds * q
            dv[e] = dv[e] + probs[e] * dm
        dqkv_ref[row(c), 0:dh] = dq.astype(bf16)
    for c in range(positions):
        dqkv_ref[row(c), dh : 2 * dh] = dk[c].astype(bf16)
        dqkv_ref[row(c), 2 * dh :] = dv[c].astype(bf16)

    @pl.loop(0, 3 * dh // tile, unroll=6)
    def _(j):
        cols = pl.ds(pl.multiple_of(j * tile, tile), tile)
        part_qkv = dot(n_t_ref[...], dqkv_ref[:, cols]).astype(bf16)
        stage_ref[...] = part_qkv.reshape(owners, 2, rows_qkv, tile)
        keep_ref[:, :, cols] = stage_ref[:, side]
        send_ref[:, :, cols] = stage_ref[:, 1 - side]


def pack_body(query_hbm, keys_hbm, values_hbm, o_hbm, in_ref, out_ref, in_sems, out_sems):
    sources = (query_hbm, keys_hbm, values_hbm)
    loads = [pltpu.make_async_copy(s.at[0], in_ref.at[k], in_sems.at[k]) for k, s in enumerate(sources)]
    stores = [
        pltpu.make_async_copy(out_ref.at[:, k], o_hbm.at[:, k], out_sems.at[k]) for k in range(len(sources))
    ]
    for load in loads:
        load.start()
    width = out_ref.shape[3]
    for k in range(len(sources)):
        loads[k].wait()
        for d in range(out_ref.shape[0]):
            out_ref[d, k] = in_ref[k, :, d * width : (d + 1) * width]
        stores[k].start()
    for store in stores:
        store.wait()


def add_cut_body(a_ref, b_ref, o_ref):
    width = o_ref.shape[3]
    for k in range(o_ref.shape[1]):
        cols = slice(k * width, (k + 1) * width)
        o_ref[:, k] = (a_ref[:, :, cols].astype(f32) + b_ref[:, :, cols].astype(f32)).astype(bf16)


def fold_cut_body(x_ref, o_ref):
    width = o_ref.shape[2]
    for j in range(o_ref.shape[0]):
        cols = slice(j * width, (j + 1) * width)
        o_ref[j] = functools.reduce(
            jnp.add, [x_ref[d, :, cols].astype(f32) for d in range(x_ref.shape[0])]
        ).astype(bf16)


def fold_copy_body(x_ref, o_ref):
    total = functools.reduce(jnp.add, [x_ref[d].astype(f32) for d in range(x_ref.shape[0])])
    for j in range(o_ref.shape[0]):
        o_ref[j] = total.astype(bf16)


def lay_out_body(x_ref, qkv_ref, out_ref):
    width = x_ref.shape[2]
    rows_out, cols_out = out_ref.shape
    for j in range(x_ref.shape[0]):
        part, at = x_ref[j].astype(f32), j * width
        if at < qkv_ref.shape[1]:
            qkv_ref[:, at : at + width] = part
        else:
            at -= qkv_ref.shape[1]
            for k in range(2):
                cols = slice(k * (cols_out // 2) + at, k * (cols_out // 2) + at + width)
                out_ref[:, cols] = part[k * rows_out : (k + 1) * rows_out]


VMEM = pl.BlockSpec(memory_space=pltpu.VMEM)
SMEM = pl.BlockSpec(memory_space=pltpu.SMEM)
HBM = pl.BlockSpec(memory_space=pltpu.HBM)


def kernel(body, outs, name, flops, in_specs=None, out_specs=None, scratch=(), room=None):
    many = isinstance(outs, (list, tuple))
    every = list(outs) if many else [outs]
    size = sum(math.prod(o.shape) * o.dtype.itemsize for o in every)

    def call(*args):
        return pl.pallas_call(
            body,
            out_shape=every if many else outs,
            in_specs=in_specs or [VMEM] * len(args),
            out_specs=out_specs or ([VMEM] * len(every) if many else VMEM),
            scratch_shapes=list(scratch),
            cost_estimate=pl.CostEstimate(
                flops=flops,
                bytes_accessed=size + sum(math.prod(a.shape) * a.dtype.itemsize for a in args),
                transcendentals=0,
            ),
            compiler_params=pltpu.CompilerParams(vmem_limit_bytes=room),
            name=name,
        )(*args)

    return call


def shape(dims, dtype=bf16):
    return jax.ShapeDtypeStruct(tuple(dims), dtype)


def to_all(x, axis):
    return lax.all_to_all(x, axis, 0, 0, tiled=True)


def turned(x, axis, k):
    n = lax.axis_size(axis)
    return lax.ppermute(x, axis, [(i, (i + k) % n) for i in range(n)])


def depth_call(weight, place, attended, embedded, codes, gain, w_in, table, weights):
    frames, positions = codes.shape
    width, entries, rows = w_in.shape[1], table.shape[0], frames * positions
    dh = (weights[0].shape[1] - width // 2) // 3
    share, columns = weights[0].shape
    owners = len(weights) // 2
    cut = shape((owners, share, columns))
    pairs = len(pairs_of(positions)) * frames
    return kernel(
        functools.partial(depth_body, weight=weight, head=DEPTH_HEAD),
        (cut, cut),
        "depth",
        11 * 10**9,
        room=42 << 20,
        in_specs=[SMEM] + [VMEM] * 3 + [HBM] * (3 + len(weights)),
        scratch=[
            pltpu.VMEM(embedded.shape, bf16),
            pltpu.VMEM(w_in.shape, bf16),
            pltpu.VMEM(table.shape, bf16),
            pltpu.VMEM((width, columns), bf16),
            pltpu.VMEM((dh, width), bf16),
            pltpu.VMEM((rows, width), f32),
            pltpu.VMEM((rows, width), bf16),
            pltpu.VMEM((width, rows), bf16),
            pltpu.VMEM((rows, 3 * dh), bf16),
            pltpu.VMEM((pairs, 2 * dh), bf16),
            pltpu.VMEM((pairs, dh), f32),
            pltpu.VMEM((pairs, dh), f32),
            pltpu.VMEM((rows, dh), bf16),
            pltpu.VMEM((dh, rows), bf16),
            pltpu.VMEM((rows, 128), f32),
            pltpu.VMEM((rows, entries), f32),
            pltpu.VMEM((rows, entries), bf16),
            pltpu.VMEM((rows, width), bf16),
            pltpu.VMEM((rows, 3 * dh), bf16),
            pltpu.VMEM((owners, 2, share, 256), bf16),
            pltpu.SemaphoreType.DMA((2 * owners,)),
            pltpu.SemaphoreType.DMA((width // 256,)),
            pltpu.SemaphoreType.DMA,
            pltpu.SemaphoreType.DMA,
        ],
    )(place, attended, codes, gain.reshape(1, width), embedded, w_in, table, *weights)


def local(query, keys, values, codes, w_in, table, gain, w_qkv, w_out):
    parts = lax.axis_size(CTX)
    frames, positions = codes.shape[1:]
    width, dh = w_in.shape[1], w_out.shape[0] * lax.axis_size(DP)
    entries = table.shape[0]
    place = jnp.stack([lax.axis_index(name) for name in DP])

    blocks = (parts, 3, frames, HEAD_DIM)
    packed = kernel(
        pack_body,
        shape(blocks),
        "pack",
        1 << 20,
        in_specs=[HBM] * 3,
        out_specs=HBM,
        scratch=[
            pltpu.VMEM((3, *query.shape[1:]), bf16),
            pltpu.VMEM(blocks, bf16),
            pltpu.SemaphoreType.DMA((3,)),
            pltpu.SemaphoreType.DMA((3,)),
        ],
    )(query, keys, values)
    w_qkv, w_out, packed = lax.optimization_barrier((w_qkv, w_out, packed))
    both = jnp.concatenate(
        [w_qkv, jnp.concatenate([w_out[:, : width // 2], w_out[:, width // 2 :]], axis=0)], axis=1
    )
    embedded = kernel(
        embed_body,
        shape((positions - 1, frames, width)),
        "embed",
        2 * (positions - 1) * frames * entries * width,
        room=10 << 20,
        scratch=[pltpu.VMEM(((positions - 1) * frames, entries), bf16)],
    )(codes[0], table)
    other, embedded = lax.optimization_barrier((turned(both, "dp_0", 1), embedded))
    ring = lax.axis_size("dp_1")
    weights = [w if k == 0 else turned(w, "dp_1", k) for w in (both, other) for k in range(ring)]
    weights += [turned(w, "dp_2", 1) for w in weights]

    moved = to_all(packed, CTX)
    moved, embedded, weights, place = lax.optimization_barrier((moved, embedded, weights, place))

    heads = kernel(
        functools.partial(attend_body, step=2),
        shape((parts, frames, HEAD_DIM)),
        "attend",
        4 * (parts * frames) ** 2 * HEAD_DIM,
        room=24 << 20,
    )(moved)
    attended = to_all(heads, CTX)

    keep, send = depth_call(
        1.0 / lax.axis_size(DP), place, attended, embedded, codes[0], gain, w_in, table, weights
    )
    swapped = turned(send, "dp_2", 1)
    owners, rows, columns = keep.shape
    planes, lane = lax.axis_size("ctx_0"), columns // parts
    halves = shape((owners, planes, rows, columns // planes))
    chip_sum = kernel(add_cut_body, halves, "chip_sum", 1 << 22, room=16 << 20)(keep, swapped)
    chip_sum = chip_sum.reshape(owners * planes, rows, columns // planes)
    plane_sum = kernel(
        fold_cut_body, shape((parts // planes, rows, lane)), "plane_sum", 1 << 22, room=8 << 20
    )(to_all(chip_sum, PLANE))
    whole_sum = kernel(fold_copy_body, shape((parts, rows, lane)), "whole_sum", 1 << 20, room=4 << 20)(
        to_all(plane_sum, "ctx_1")
    )
    return kernel(
        lay_out_body, (shape(w_qkv.shape, f32), shape(w_out.shape, f32)), "lay_out", 1 << 20, room=4 << 20
    )(to_all(whole_sum, CTX))


def solution(mesh):
    torus = Mesh(mesh.devices.reshape(2, 4, 2, 2, 8), DP + CTX)
    frames = P(DP, CTX, None)
    in_specs = (frames, frames, frames, frames, P(), P(), P(), P(DP, None), P(DP, None))
    out_specs = (P(DP, None), P(DP, None))
    return jax.shard_map(local, mesh=torus, in_specs=in_specs, out_specs=out_specs, check_vma=False)
```

```python
import functools
import math

import jax
import jax.numpy as jnp
from jax import lax
from jax.experimental import pallas as pl
from jax.experimental.pallas import tpu as pltpu
from jax.sharding import Mesh
from jax.sharding import PartitionSpec as P

HEAD_DIM = 128
DEPTH_HEAD = 64
DP = ("dp_0", "dp_1", "dp_2")
CTX = ("ctx_0", "ctx_1")
PLANE = ("dp_0", "dp_1", "ctx_0")

bf16, f32 = jnp.bfloat16, jnp.float32
NEG = -1e30
EPS = 1e-6
NT = (((1,), (1,)), ((), ()))


def dot(a, b):
    return jnp.dot(a, b, preferred_element_type=f32)


def dot_nt(a, b):
    return lax.dot_general(a, b, NT, preferred_element_type=f32)


def attend_body(x_ref, o_ref, *, step):
    blocks, _, rows, dim = x_ref.shape
    for i in range(0, blocks, step):
        seen = i + step
        q = x_ref[i:seen, 0].reshape(step * rows, dim)
        k = x_ref[0:seen, 1].reshape(seen * rows, dim)
        v = x_ref[0:seen, 2].reshape(seen * rows, dim)
        s = dot_nt(q, k)
        shape = (step * rows, step * rows)
        ok = lax.broadcasted_iota(jnp.int32, shape, 1) <= lax.broadcasted_iota(jnp.int32, shape, 0)
        last = jnp.where(ok, s[:, i * rows :], NEG)
        s = last if i == 0 else jnp.concatenate([s[:, : i * rows], last], axis=1)
        p = jnp.exp2((s - jnp.max(s, axis=1, keepdims=True)) * (math.log2(math.e) / math.sqrt(dim)))
        total = jnp.sum(p, axis=1, keepdims=True)
        out = dot(p.astype(bf16), v) / total
        o_ref[i:seen] = out.astype(bf16).reshape(step, rows, dim)


def embed_body(codes_ref, table_ref, o_ref, hot_ref):
    count, frames, width = o_ref.shape
    entries = table_ref.shape[0]
    ids = lax.broadcasted_iota(jnp.int32, (frames, entries), 1)
    for c in range(count):
        hot_ref[c * frames : (c + 1) * frames] = (
            (ids == codes_ref[:, c : c + 1]).astype(f32).astype(bf16)
        )
    tile = 256

    @pl.loop(0, width // tile)
    def _(j):
        cols = pl.ds(pl.multiple_of(j * tile, tile), tile)
        rows = dot(hot_ref[...], table_ref[:, cols])
        o_ref[:, :, cols] = rows.astype(bf16).reshape(count, frames, tile)


def put_split(ref, rows, term, width):
    high = term.astype(bf16)
    low = (term - high.astype(f32)).astype(bf16)
    for j in range(term.shape[1] // width):
        cols = slice(j * width, (j + 1) * width)
        ref[rows, 2 * j * width : (2 * j + 1) * width] = high[:, cols]
        ref[rows, (2 * j + 1) * width : (2 * j + 2) * width] = low[:, cols]


def head_sums(ref, heads_block, store):
    depth, width = heads_block.shape
    for j in range(ref.shape[1] // depth):
        store(
            slice(j * width, (j + 1) * width),
            dot(ref[:, j * depth : (j + 1) * depth], heads_block),
        )


def same_head(width, head):
    r = lax.broadcasted_iota(jnp.int32, (width, width), 0) // head
    c = lax.broadcasted_iota(jnp.int32, (width, width), 1) // head
    return (r == c).astype(f32).astype(bf16)


def pairs_of(positions):
    return [(c, e) for c in range(positions) for e in range(c + 1)]


def depth_body(*refs, weight, head):
    place_ref, att_ref, codes_ref, gain_ref, emb_hbm, w_in_hbm, table_hbm = refs[:7]
    shards = refs[7:-26]
    keep_ref, send_ref, emb_ref, w_in_ref, table_ref, w_ref, w_out_ref, x_ref, n_ref = refs[-26:-17]
    n_t_ref, qkv_ref, term_ref, s_ref, p_ref, mix_ref, mix_t_ref, inv_ref = refs[-17:-9]
    logit_ref, g_ref, dr_ref, dqkv_ref, stage_ref, sems, in_sems, emb_sem, table_sem = refs[-9:]
    frames, positions = codes_ref.shape
    width = x_ref.shape[1]
    entries = table_ref.shape[0]
    dh = w_out_ref.shape[0]
    owners, _, rows_qkv, _ = stage_ref.shape
    rows_out = rows_qkv // 2
    half = width // 2
    tile = 256
    side = place_ref[2]
    z_ref = x_ref
    dz_ref = logit_ref.at[:, :width]
    dmix_ref = logit_ref.at[:, width : width + dh]
    row = lambda c: pl.ds(c * frames, frames)

    tile_cols = lambda j: pl.ds(pl.multiple_of(j * tile, tile), tile)
    load_in = lambda j: pltpu.make_async_copy(
        w_in_hbm.at[:, tile_cols(j)], w_in_ref.at[:, tile_cols(j)], in_sems.at[j]
    )
    load_emb = pltpu.make_async_copy(emb_hbm, emb_ref, emb_sem)
    load_table = pltpu.make_async_copy(table_hbm, table_ref, table_sem)
    load_in(0).start()
    load_emb.start()
    for j in range(1, width // tile):
        load_in(j).start()
    loads = []
    ring = len(shards) // 4
    for k, ref in enumerate(shards):
        twin, plane, back = k // (2 * ring), k // ring % 2, k % ring
        at = (place_ref[0] + plane) % 2
        at = at * ring + (place_ref[1] + ring - back) % ring
        at = at * 2 + (side + twin) % 2
        rows = pl.ds(pl.multiple_of(at * rows_qkv, rows_qkv), rows_qkv)
        loads.append(pltpu.make_async_copy(ref, w_ref.at[rows], sems.at[k]))
    load_emb.wait()
    for j in range(width // tile):
        load_in(j).wait()
        if j == 1:
            for load in loads:
                load.start()
    att = jnp.concatenate([att_ref[h] for h in range(att_ref.shape[0])], axis=1)

    @pl.loop(0, width // tile, unroll=4)
    def _(j):
        cols = pl.ds(pl.multiple_of(j * tile, tile), tile)
        hidden = dot(att, w_in_ref[:, cols])
        x_ref[row(0), cols] = hidden
        for c in range(1, positions):
            x_ref[row(c), cols] = hidden + emb_ref[c - 1, :, cols].astype(f32)

    for c in range(positions):
        x = x_ref[row(c), :]
        scale = lax.rsqrt(jnp.mean(x * x, axis=1, keepdims=True) + EPS)
        normed = (x * scale * gain_ref[...]).astype(bf16)
        n_ref[row(c), :] = normed
        n_t_ref[:, row(c)] = normed.T

    for load in loads:
        load.wait()
    load_table.start()
    for d in range(2 * owners):
        for k in range(2):
            w_out_ref[d * rows_out : (d + 1) * rows_out, k * half : (k + 1) * half] = w_ref[
                d * rows_qkv + k * rows_out : d * rows_qkv + (k + 1) * rows_out, 3 * dh :
            ]

    @pl.loop(0, 3 * dh // tile, unroll=6)
    def _(j):
        cols = pl.ds(pl.multiple_of(j * tile, tile), tile)
        qkv_ref[:, cols] = dot(n_ref[...], w_ref[:, cols]).astype(bf16)

    block = jnp.concatenate([same_head(tile, head)] * 2, axis=0)
    scale = 1.0 / math.sqrt(head)
    pairs = pairs_of(positions)
    part = lambda c, k: qkv_ref[row(c), k * dh : (k + 1) * dh].astype(f32)
    pair = lambda c, e: pl.ds(pairs.index((c, e)) * frames, frames)

    def store_scores(cols, values):
        s_ref[:, cols] = values * scale

    for c, e in pairs:
        put_split(term_ref, pair(c, e), part(c, 0) * part(e, 1), tile)
    head_sums(term_ref, block, store_scores)
    for c in range(positions):
        scores = [s_ref[pair(c, e), :] for e in range(c + 1)]
        top = functools.reduce(jnp.maximum, scores)
        raised = [jnp.exp(s - top) for s in scores]
        fraction = 1.0 / functools.reduce(jnp.add, raised)
        mixed = jnp.zeros((frames, dh), f32)
        for e in range(c + 1):
            p = raised[e] * fraction
            p_ref[pair(c, e), :] = p
            mixed = mixed + p * part(e, 2)
        mixed = mixed.astype(bf16)
        mix_ref[row(c), :] = mixed
        mix_t_ref[:, row(c)] = mixed.T

    @pl.loop(0, width // tile, unroll=4)
    def _(j):
        cols = pl.ds(pl.multiple_of(j * tile, tile), tile)
        z_ref[:, cols] = x_ref[:, cols] + dot(mix_ref[...], w_out_ref[:, cols])

    for c in range(positions):
        r = z_ref[row(c), :]
        inv = lax.rsqrt(jnp.mean(r * r, axis=1, keepdims=True) + EPS)
        inv_ref[row(c), :] = jnp.broadcast_to(inv, (frames, inv_ref.shape[1]))
        z = r * inv
        z_ref[row(c), :] = z
        dr_ref[row(c), :] = z.astype(bf16)

    load_table.wait()

    @pl.loop(0, entries // tile, unroll=8)
    def _(j):
        cols = pl.ds(pl.multiple_of(j * tile, tile), tile)
        logit_ref[:, cols] = dot_nt(dr_ref[...], table_ref[cols, :])

    ids = lax.broadcasted_iota(jnp.int32, (frames, entries), 1)
    for c in range(positions):
        s = logit_ref[row(c), :]
        e = jnp.exp(s - jnp.max(s, axis=1, keepdims=True))
        total = jnp.sum(e, axis=1, keepdims=True)
        hit = jnp.where(ids == codes_ref[:, c : c + 1], weight, 0.0)
        g_ref[row(c), :] = (e * (weight / total) - hit).astype(bf16)

    @pl.loop(0, width // tile, unroll=4)
    def _(j):
        cols = pl.ds(pl.multiple_of(j * tile, tile), tile)
        dz_ref[:, cols] = dot(g_ref[...], table_ref[:, cols])

    for c in range(positions):
        dz, z = dz_ref[row(c), :], z_ref[row(c), :]
        along = jnp.mean(dz * z, axis=1, keepdims=True)
        dr_ref[row(c), :] = (inv_ref[row(c), 0:1] * (dz - z * along)).astype(bf16)

    for j in range(width // tile):
        part_out = dot(mix_t_ref[...], dr_ref[:, j * tile : (j + 1) * tile]).astype(bf16)
        stage_ref[:, :, 0:rows_out, :] = part_out.reshape(owners, 2, rows_out, tile)
        k, at = divmod(j * tile, half)
        rows = slice(k * rows_out, (k + 1) * rows_out)
        cols = slice(3 * dh + at, 3 * dh + at + tile)
        keep_ref[:, rows, cols] = stage_ref[:, side, 0:rows_out, :]
        send_ref[:, rows, cols] = stage_ref[:, 1 - side, 0:rows_out, :]

    @pl.loop(0, dh // tile, unroll=2)
    def _(j):
        cols = pl.ds(pl.multiple_of(j * tile, tile), tile)
        dmix_ref[:, cols] = dot_nt(dr_ref[...], w_out_ref[cols, :])

    def store_plain(cols, values):
        s_ref[:, cols] = values

    for c, e in pairs:
        put_split(term_ref, pair(c, e), dmix_ref[row(c), :] * part(e, 2), tile)
    head_sums(term_ref, block, store_plain)
    dk = [jnp.zeros((frames, dh), f32) for _ in range(positions)]
    dv = [jnp.zeros((frames, dh), f32) for _ in range(positions)]
    for c in range(positions):
        dm = dmix_ref[row(c), :]
        probs = [p_ref[pair(c, e), :] for e in range(c + 1)]
        dprobs = [s_ref[pair(c, e), :] for e in range(c + 1)]
        along = functools.reduce(jnp.add, [d * p for d, p in zip(dprobs, probs)])
        q = part(c, 0)
        dq = jnp.zeros((frames, dh), f32)
        for e in range(c + 1):
            ds = probs[e] * (dprobs[e] - along) * scale
            dq = dq + ds * part(e, 1)
            dk[e] = dk[e] + ds * q
            dv[e] = dv[e] + probs[e] * dm
        dqkv_ref[row(c), 0:dh] = dq.astype(bf16)
    for c in range(positions):
        dqkv_ref[row(c), dh : 2 * dh] = dk[c].astype(bf16)
        dqkv_ref[row(c), 2 * dh :] = dv[c].astype(bf16)

    @pl.loop(0, 3 * dh // tile, unroll=6)
    def _(j):
        cols = pl.ds(pl.multiple_of(j * tile, tile), tile)
        part_qkv = dot(n_t_ref[...], dqkv_ref[:, cols]).astype(bf16)
        stage_ref[...] = part_qkv.reshape(owners, 2, rows_qkv, tile)
        keep_ref[:, :, cols] = stage_ref[:, side]
        send_ref[:, :, cols] = stage_ref[:, 1 - side]


def pack_body(query_hbm, keys_hbm, values_hbm, o_hbm, in_ref, out_ref, in_sems, out_sems):
    sources = (query_hbm, keys_hbm, values_hbm)
    loads = [pltpu.make_async_copy(s.at[0], in_ref.at[k], in_sems.at[k]) for k, s in enumerate(sources)]
    stores = [
        pltpu.make_async_copy(out_ref.at[:, k], o_hbm.at[:, k], out_sems.at[k]) for k in range(len(sources))
    ]
    for load in loads:
        load.start()
    width = out_ref.shape[3]
    for k in range(len(sources)):
        loads[k].wait()
        for d in range(out_ref.shape[0]):
            out_ref[d, k] = in_ref[k, :, d * width : (d + 1) * width]
        stores[k].start()
    for store in stores:
        store.wait()


def add_cut_body(a_ref, b_ref, o_ref):
    width = o_ref.shape[3]
    for k in range(o_ref.shape[1]):
        cols = slice(k * width, (k + 1) * width)
        o_ref[:, k] = (a_ref[:, :, cols].astype(f32) + b_ref[:, :, cols].astype(f32)).astype(bf16)


def fold_cut_body(x_ref, o_ref):
    width = o_ref.shape[2]
    for j in range(o_ref.shape[0]):
        cols = slice(j * width, (j + 1) * width)
        o_ref[j] = functools.reduce(
            jnp.add, [x_ref[d, :, cols].astype(f32) for d in range(x_ref.shape[0])]
        ).astype(bf16)


def fold_copy_body(x_ref, o_ref):
    total = functools.reduce(jnp.add, [x_ref[d].astype(f32) for d in range(x_ref.shape[0])])
    for j in range(o_ref.shape[0]):
        o_ref[j] = total.astype(bf16)


def lay_out_body(x_ref, qkv_ref, out_ref):
    width = x_ref.shape[2]
    rows_out, cols_out = out_ref.shape
    for j in range(x_ref.shape[0]):
        part, at = x_ref[j].astype(f32), j * width
        if at < qkv_ref.shape[1]:
            qkv_ref[:, at : at + width] = part
        else:
            at -= qkv_ref.shape[1]
            for k in range(2):
                cols = slice(k * (cols_out // 2) + at, k * (cols_out // 2) + at + width)
                out_ref[:, cols] = part[k * rows_out : (k + 1) * rows_out]


VMEM = pl.BlockSpec(memory_space=pltpu.VMEM)
SMEM = pl.BlockSpec(memory_space=pltpu.SMEM)
HBM = pl.BlockSpec(memory_space=pltpu.HBM)


def kernel(body, outs, name, flops, in_specs=None, out_specs=None, scratch=(), room=None):
    many = isinstance(outs, (list, tuple))
    every = list(outs) if many else [outs]
    size = sum(math.prod(o.shape) * o.dtype.itemsize for o in every)

    def call(*args):
        return pl.pallas_call(
            body,
            out_shape=every if many else outs,
            in_specs=in_specs or [VMEM] * len(args),
            out_specs=out_specs or ([VMEM] * len(every) if many else VMEM),
            scratch_shapes=list(scratch),
            cost_estimate=pl.CostEstimate(
                flops=flops,
                bytes_accessed=size + sum(math.prod(a.shape) * a.dtype.itemsize for a in args),
                transcendentals=0,
            ),
            compiler_params=pltpu.CompilerParams(vmem_limit_bytes=room),
            name=name,
        )(*args)

    return call


def shape(dims, dtype=bf16):
    return jax.ShapeDtypeStruct(tuple(dims), dtype)


def to_all(x, axis):
    return lax.all_to_all(x, axis, 0, 0, tiled=True)


def turned(x, axis, k):
    n = lax.axis_size(axis)
    return lax.ppermute(x, axis, [(i, (i + k) % n) for i in range(n)])


def depth_call(weight, place, attended, embedded, codes, gain, w_in, table, weights):
    frames, positions = codes.shape
    width, entries, rows = w_in.shape[1], table.shape[0], frames * positions
    dh = (weights[0].shape[1] - width // 2) // 3
    share, columns = weights[0].shape
    owners = len(weights) // 2
    cut = shape((owners, share, columns))
    pairs = len(pairs_of(positions)) * frames
    return kernel(
        functools.partial(depth_body, weight=weight, head=DEPTH_HEAD),
        (cut, cut),
        "depth",
        11 * 10**9,
        room=42 << 20,
        in_specs=[SMEM] + [VMEM] * 3 + [HBM] * (3 + len(weights)),
        scratch=[
            pltpu.VMEM(embedded.shape, bf16),
            pltpu.VMEM(w_in.shape, bf16),
            pltpu.VMEM(table.shape, bf16),
            pltpu.VMEM((width, columns), bf16),
            pltpu.VMEM((dh, width), bf16),
            pltpu.VMEM((rows, width), f32),
            pltpu.VMEM((rows, width), bf16),
            pltpu.VMEM((width, rows), bf16),
            pltpu.VMEM((rows, 3 * dh), bf16),
            pltpu.VMEM((pairs, 2 * dh), bf16),
            pltpu.VMEM((pairs, dh), f32),
            pltpu.VMEM((pairs, dh), f32),
            pltpu.VMEM((rows, dh), bf16),
            pltpu.VMEM((dh, rows), bf16),
            pltpu.VMEM((rows, 128), f32),
            pltpu.VMEM((rows, entries), f32),
            pltpu.VMEM((rows, entries), bf16),
            pltpu.VMEM((rows, width), bf16),
            pltpu.VMEM((rows, 3 * dh), bf16),
            pltpu.VMEM((owners, 2, share, 256), bf16),
            pltpu.SemaphoreType.DMA((2 * owners,)),
            pltpu.SemaphoreType.DMA((width // 256,)),
            pltpu.SemaphoreType.DMA,
            pltpu.SemaphoreType.DMA,
        ],
    )(place, attended, codes, gain.reshape(1, width), embedded, w_in, table, *weights)


def local(query, keys, values, codes, w_in, table, gain, w_qkv, w_out):
    parts = lax.axis_size(CTX)
    frames, positions = codes.shape[1:]
    width, dh = w_in.shape[1], w_out.shape[0] * lax.axis_size(DP)
    entries = table.shape[0]
    place = jnp.stack([lax.axis_index(name) for name in DP])

    blocks = (parts, 3, frames, HEAD_DIM)
    packed = kernel(
        pack_body,
        shape(blocks),
        "pack",
        1 << 20,
        in_specs=[HBM] * 3,
        out_specs=HBM,
        scratch=[
            pltpu.VMEM((3, *query.shape[1:]), bf16),
            pltpu.VMEM(blocks, bf16),
            pltpu.SemaphoreType.DMA((3,)),
            pltpu.SemaphoreType.DMA((3,)),
        ],
    )(query, keys, values)
    w_qkv, w_out, packed = lax.optimization_barrier((w_qkv, w_out, packed))
    both = jnp.concatenate(
        [w_qkv, jnp.concatenate([w_out[:, : width // 2], w_out[:, width // 2 :]], axis=0)], axis=1
    )
    embedded = kernel(
        embed_body,
        shape((positions - 1, frames, width)),
        "embed",
        2 * (positions - 1) * frames * entries * width,
        room=10 << 20,
        scratch=[pltpu.VMEM(((positions - 1) * frames, entries), bf16)],
    )(codes[0], table)
    other, embedded = lax.optimization_barrier((turned(both, "dp_0", 1), embedded))
    ring = lax.axis_size("dp_1")
    weights = [w if k == 0 else turned(w, "dp_1", k) for w in (both, other) for k in range(ring)]
    weights += [turned(w, "dp_2", 1) for w in weights]

    moved = to_all(packed, CTX)
    moved, embedded, weights, place = lax.optimization_barrier((moved, embedded, weights, place))

    heads = kernel(
        functools.partial(attend_body, step=2),
        shape((parts, frames, HEAD_DIM)),
        "attend",
        4 * (parts * frames) ** 2 * HEAD_DIM,
        room=24 << 20,
    )(moved)
    attended = to_all(heads, CTX)

    keep, send = depth_call(
        1.0 / lax.axis_size(DP), place, attended, embedded, codes[0], gain, w_in, table, weights
    )
    swapped = turned(send, "dp_2", 1)
    owners, rows, columns = keep.shape
    planes, lane = lax.axis_size("ctx_0"), columns // parts
    halves = shape((owners, planes, rows, columns // planes))
    chip_sum = kernel(add_cut_body, halves, "chip_sum", 1 << 22, room=16 << 20)(keep, swapped)
    chip_sum = chip_sum.reshape(owners * planes, rows, columns // planes)
    plane_sum = kernel(
        fold_cut_body, shape((parts // planes, rows, lane)), "plane_sum", 1 << 22, room=8 << 20
    )(to_all(chip_sum, PLANE))
    whole_sum = kernel(fold_copy_body, shape((parts, rows, lane)), "whole_sum", 1 << 20, room=4 << 20)(
        to_all(plane_sum, "ctx_1")
    )
    return kernel(
        lay_out_body, (shape(w_qkv.shape, f32), shape(w_out.shape, f32)), "lay_out", 1 << 20, room=4 << 20
    )(to_all(whole_sum, CTX))


def solution(mesh):
    torus = Mesh(mesh.devices.reshape(2, 4, 2, 2, 8), DP + CTX)
    frames = P(DP, CTX, None)
    in_specs = (frames, frames, frames, frames, P(), P(), P(), P(DP, None), P(DP, None))
    out_specs = (P(DP, None), P(DP, None))
    return jax.shard_map(local, mesh=torus, in_specs=in_specs, out_specs=out_specs, check_vma=False)
```
